512 devices in a mesh: slab: 128 (over y, z, core), sub: 4 (over x).
Axes of the slice: x: 4, y: 8, z: 8, core: 2. Of those that a mesh axis runs over, the one named last changes fastest.
Arguments:
- orbitals: bfloat16 [512, 16, 110592], P(('slab', 'sub')), may hold values from -0.25 to 0.25
- occupations: int32 [512, 16], P(('slab', 'sub')), may hold values from 0 to 2, as said below
- patch_sign: int32 [512], P(('slab', 'sub')), may hold values from -1 to 1, as said below
- corners: int32 [512, 3], replicated, may hold values from 0 to 511, as said below
- core_span: int32 [512, 6], P(('slab', 'sub')), may hold values from 8 to 32, as said below
- outer_density: float32 [512, 256, 256], P('slab', 'sub'), may hold values from 0 to 0.3, as said below
Outputs:
- box_potential: float32 [512, 110592], P(('slab', 'sub'))
- potential: float32 [512, 256, 256], P('slab', 'sub')
The draws below stay inside these ranges and needn't reach their ends.
Inputs may be any that keep to these rules, and one draw needn't show every extreme that they name: Each fragment's occupations sum to 16. patch_sign[f] is -1 raised to the number of dimensions along which fragment f's core is 16 cells long. corners[f, 0] lies in [4 * (f // 4), that + 4), the planes of the slab index that holds fragment f; corners[f, 1] lies in [0, 256) and corners[f, 2] in [0, 256). `core_span`: each core lies inside its box and is 16 or 32 cells long along each dimension; fragments 8 j to 8 j + 7 are the eight kinds of core that start at one common grid cell, a corner of the fragment division; along the second and third dimensions these corners lie at different points of one lattice of spacing 16. `outer_density`: nonnegative; zero exactly on the cells where the fragments given here have signed coverage one.
All inputs are finite; a program needn't handle non-finite values.
Results may differ from the reference program's by a relative error of at most 0.0003.
Values sent between devices are 32-bit elements; how exact they have to be, the bound alone decides.
A program may use at most 64 MiB of HBM per device.

```python
import math
import jax
import jax.numpy as jnp
from jax import lax

BOX = 48
ORB = 16
NX = 256
NY = 256
Z_DEV = 4
NZ = 512
FRAGS = 512


def fragment_layout(key):
    base = jax.random.fold_in(key, 11)
    keys = jax.random.split(base, 4)
    piece = BOX // 3
    half = piece // 2
    pairs = FRAGS // 8
    pair_index = jnp.arange(pairs, dtype=jnp.int32)
    upper = Z_DEV * (2 * pair_index + 1) + jax.random.randint(keys[0], (pairs,), 0, Z_DEV, dtype=jnp.int32)
    across = NY // piece
    slots = jax.random.permutation(keys[1], NX // piece * across)[:pairs].astype(jnp.int32)
    offsets = jax.random.randint(keys[2], (2,), 0, piece, dtype=jnp.int32)
    core_x = slots // across * piece + offsets[0]
    core_y = slots % across * piece + offsets[1]
    kind_keys = jax.random.split(keys[3], FRAGS // 4)
    orders = jax.vmap(lambda k: jax.random.permutation(k, 4))(kind_keys).astype(jnp.int32).reshape(FRAGS)
    fragment = jnp.arange(FRAGS, dtype=jnp.int32)
    slab_index = fragment // 4
    owner = slab_index // 2
    thick_z = 1 + slab_index % 2
    thick_x = 1 + orders // 2
    thick_y = 1 + orders % 2
    start_z = jnp.where(thick_z == 2, upper[owner], upper[owner] - Z_DEV)
    first_z = jnp.where(thick_z == 2, half, half + Z_DEV)
    first_x = jnp.where(thick_x == 2, half, piece)
    first_y = jnp.where(thick_y == 2, half, piece)
    start_x = (core_x[owner] - first_x) % NX
    start_y = (core_y[owner] - first_y) % NY
    signs = (2 * thick_z - 3) * (2 * thick_x - 3) * (2 * thick_y - 3)
    corner_table = jnp.stack([start_z, start_x, start_y], axis=1).astype(jnp.int32)
    span_table = jnp.stack([first_z, first_x, first_y, piece * thick_z, piece * thick_x, piece * thick_y], axis=1).astype(jnp.int32)
    return (corner_table, span_table, signs.astype(jnp.int32), upper + half, core_x, core_y)


def draw_corners(key, part):
    return fragment_layout(key)[0]


def draw_core_span(key, part):
    return fragment_layout(key)[1]


def draw_patch_sign(key, part):
    return fragment_layout(key)[2]


def draw_occupations(key, part):
    keys = jax.random.split(jax.random.fold_in(key, 23), FRAGS + 1)
    ranks = jax.vmap(lambda k: jax.random.permutation(k, ORB))(keys[:FRAGS]).astype(jnp.int32)
    doubled = jax.random.randint(keys[FRAGS], (FRAGS, 1), 1, ORB // 2 + 1, dtype=jnp.int32)
    filled = jnp.where(ranks < doubled, 2, jnp.where(ranks < 2 * doubled, 0, 1))
    return filled.astype(jnp.int32)


def cover_factor(first, count, piece):
    cells = jnp.arange(count, dtype=jnp.int32)
    distance = (cells[None, :] - first[:, None]) % count

    def hits(length):
        return jnp.where(distance < length, (length - 1 - distance) // count + 1, 0)
    return (hits(2 * piece) - hits(piece)).astype(jnp.float32)


def draw_outer_density(key, part):
    layout = fragment_layout(key)
    piece = BOX // 3
    pairs = FRAGS // 8
    factor_z = cover_factor(layout[3], NZ, piece)
    factor_x = cover_factor(layout[4], NX, piece)
    factor_y = cover_factor(layout[5], NY, piece)
    plane = (factor_x[:, :, None] * factor_y[:, None, :]).reshape(pairs, NX * NY)
    coverage = jnp.dot(factor_z.T, plane).reshape(NZ, NX, NY)
    noise_key = jax.random.fold_in(key, 31)
    values = 0.0256 * jnp.exp(0.6 * jnp.clip(jax.random.normal(noise_key, (NZ, NX, NY), jnp.float32), -4.0, 4.0))
    return (values * (1.0 - coverage)).astype(jnp.float32)


def level_of(own_key, extent, cuts, low, top_value):
    factor_of, own = 1.0, jax.random.fold_in(own_key, 6)
    for dim, blocks in cuts:
        steps = jnp.exp(jax.random.uniform(jax.random.fold_in(own, dim), (blocks,), jnp.float32, low / len(cuts), top_value / len(cuts)))
        factor_of = factor_of * jnp.repeat(steps, extent[dim] // blocks).reshape([-1 if axis == dim else 1 for axis in range(len(extent))])
    return factor_of


def centred(rng, shape, width, limit, pieces=(), kind=jnp.bfloat16):
    level = level_of(rng, shape, pieces, -0.22, 0.18) if pieces else 1.0
    values = jax.random.normal(rng, shape, jnp.float32) * width * level
    return jnp.minimum(jnp.maximum(values, -limit), limit).astype(kind)


def setup_inputs(seed: int = 0) -> dict:
    seeds = jax.random.split(jax.random.key(seed), 7)
    return {
        "orbitals": centred(seeds[0], (FRAGS, ORB, BOX * BOX * BOX), 0.04, 0.25, ((0, 512),)),
        "occupations": draw_occupations(jax.random.fold_in(seeds[6], 71), 0),
        "patch_sign": draw_patch_sign(jax.random.fold_in(seeds[6], 71), 0),
        "corners": draw_corners(jax.random.fold_in(seeds[6], 71), 0),
        "core_span": draw_core_span(jax.random.fold_in(seeds[6], 71), 0),
        "outer_density": draw_outer_density(jax.random.fold_in(seeds[6], 71), 0),
    }


spacing = 0.35
floor_density = 0.001


def wave_squares(index, count):
    folded = jnp.where(index > count // 2, index - count, index)
    wave = (2.0 * math.pi / (count * spacing)) * folded.astype(jnp.float32)
    return wave * wave


def exchange_correlation(density):
    clipped = jnp.maximum(density, floor_density)
    radius = jnp.cbrt(3.0 / (4.0 * math.pi * clipped))
    exchange = -jnp.cbrt(3.0 * clipped / math.pi)
    correlation = -0.44 / (radius + 7.8) - 0.44 * radius / (3.0 * (radius + 7.8) ** 2)
    return exchange + correlation


def reference(orbitals, occupations, patch_sign, corners, core_span, outer_density):
    copies = (BOX - 1) // NZ + 2
    cell = jnp.arange(BOX, dtype=jnp.int32)

    def add_box(fragment, grid):
        fragment = fragment.astype(jnp.int32)
        orbital_values = orbitals[fragment].astype(jnp.float32)
        weights = occupations[fragment].astype(jnp.float32)
        box_density = patch_sign[fragment].astype(jnp.float32) * jnp.sum(weights[:, None] * orbital_values * orbital_values, axis=0)
        span = core_span[fragment].astype(jnp.int32)
        inside_z = (cell >= span[0]) & (cell < span[0] + span[3])
        inside_x = (cell >= span[1]) & (cell < span[1] + span[4])
        inside_y = (cell >= span[2]) & (cell < span[2] + span[5])
        inside = (inside_z[:, None, None] & inside_x[None, :, None] & inside_y[None, None, :]).astype(jnp.float32)
        cube = box_density.reshape(BOX, BOX, BOX) * inside
        planes = jnp.pad(cube, ((0, 0), (0, NX - BOX), (0, NY - BOX)))
        planes = jnp.roll(planes, corners[fragment, 1], axis=1)
        planes = jnp.roll(planes, corners[fragment, 2], axis=2)
        start_z = corners[fragment, 0].astype(jnp.int32)
        current = lax.dynamic_slice_in_dim(grid, start_z, BOX, 0)
        return lax.dynamic_update_slice_in_dim(grid, current + planes, start_z, 0)

    extended = lax.fori_loop(0, FRAGS, add_box, jnp.zeros((copies * NZ, NX, NY), jnp.float32))
    density = jnp.sum(extended.reshape(copies, NZ, NX, NY), axis=0) + outer_density
    square = (wave_squares(jnp.arange(NZ, dtype=jnp.int32), NZ)[:, None, None]
              + wave_squares(jnp.arange(NX, dtype=jnp.int32), NX)[None, :, None]
              + wave_squares(jnp.arange(NY, dtype=jnp.int32), NY)[None, None, :])
    safe_square = jnp.where(square > 0, square, 1.0)
    kernel = jnp.where(square > 0, 4.0 * math.pi / safe_square, 0.0)
    spectrum = jnp.fft.fftn(density)
    hartree = jnp.real(jnp.fft.ifftn(spectrum * kernel)).astype(jnp.float32)
    potential = hartree + exchange_correlation(density)
    tiled = jnp.concatenate([potential] * copies, axis=0)

    def cut_box(fragment):
        start_z = corners[fragment, 0].astype(jnp.int32)
        planes = lax.dynamic_slice_in_dim(tiled, start_z, BOX, 0)
        planes = jnp.roll(planes, -corners[fragment, 1], axis=1)
        planes = jnp.roll(planes, -corners[fragment, 2], axis=2)
        return planes[:, :BOX, :BOX].reshape(BOX * BOX * BOX)

    boxes = lax.map(cut_box, jnp.arange(FRAGS, dtype=jnp.int32))
    return boxes, potential
```

```python
import functools
import math

import jax
import jax.numpy as jnp
import numpy as np
from jax import lax
from jax.experimental import pallas as pl
from jax.experimental.pallas import tpu as pltpu
from jax.sharding import PartitionSpec as P

BOX = 48
NX = 256
NY = 256
Z_DEV = 4
SUBS = 4
CORE = 32
FIRST = 8
SPACING = 0.35
FLOOR = 0.001
NEAR = FIRST // Z_DEV
REACH = 11
SPREAD = 13
TILES = BOX * BOX // 128
MESH = pl.DeviceIdType.MESH
f32 = jnp.float32
bf16 = jnp.bfloat16


def cas_table(count):
    index = np.arange(count)
    angle = 2.0 * np.pi * ((index[:, None] * index[None, :]) % count) / count
    table = (np.cos(angle) + np.sin(angle)) / np.sqrt(count)
    high = table.astype(np.float32).astype(bf16)
    low = (table - high.astype(np.float64)).astype(np.float32).astype(bf16)
    return high, low


def split(values):
    high = values.astype(bf16)
    return high, (values - high.astype(f32)).astype(bf16)


def dot(a, b):
    return jnp.dot(a, b, preferred_element_type=f32)


def dot3(a, b):
    return dot(a[0], b[0]) + (dot(a[0], b[1]) + dot(a[1], b[0]))


def lanes(shape):
    return lax.broadcasted_iota(jnp.int32, shape, len(shape) - 1)


def rows(shape):
    return lax.broadcasted_iota(jnp.int32, shape, 0)


def core_kernel(span_ref, corner_ref, box_ref, core_ref, meta_ref):
    slab = lax.axis_index("slab")
    own = slab * SUBS + lax.axis_index("sub")
    first_z, first_x, first_y = span_ref[0], span_ref[1], span_ref[2]
    long_z, long_x, long_y = span_ref[3], span_ref[4], span_ref[5]
    offset = corner_ref[own * 3] - slab * Z_DEV
    planes = BOX - FIRST
    start = first_x * BOX + first_y
    tile, lane = start // 128, start % 128
    shape = (planes, 128)
    column = lanes(shape)
    turned = []
    for t in range(13):
        row = FIRST * TILES + jnp.minimum(tile + t, TILES - 1)
        raw = box_ref[pl.ds(row, planes, stride=TILES), :]
        turned.append(pltpu.roll(raw, (128 - lane) % 128, 1))
    chunks = [jnp.where(column < 128 - lane, turned[t], turned[t + 1]) for t in range(12)]
    plane = rows(shape) + FIRST
    within_z = (plane >= first_z) & (plane < first_z + long_z)
    core_ref[...] = jnp.zeros_like(core_ref)
    for t in range(8):
        value = jnp.zeros(shape, f32)
        for m in range(4):
            source = (4 * t + m) * BOX
            chunk, begin = source // 128, source % 128
            shift = (32 * m - begin) % 128
            piece = pltpu.roll(chunks[chunk], shift, 1)
            if begin + CORE > 128:
                after = pltpu.roll(chunks[chunk + 1], shift, 1)
                piece = jnp.where(column < 32 * m + 128 - begin, piece, after)
            value = jnp.where(column // 32 == m, piece, value)
        inside = within_z & (4 * t + column // 32 < long_x) & (column % 32 < long_y)
        core_ref[pl.ds(offset * 8 + t, planes, stride=8), :] = jnp.where(inside, value, 0.0)
    start_x = (corner_ref[own * 3 + 1] + first_x) % NX
    start_y = (corner_ref[own * 3 + 2] + first_y) % NY
    meta_ref[...] = jnp.where(lanes((8, 128)) == 0, start_x, start_y)


def wait_all(sem, ref):
    pltpu.make_async_copy(ref, ref, sem).wait()


def spread_kernel(core_ref, meta_ref, outer_ref, got_ref, told_ref, plane_ref, send, recv):
    slab, sub = lax.axis_index("slab"), lax.axis_index("sub")
    slabs = lax.axis_size("slab")

    def pass_outer(k, carry):
        target = (sub + k) % SUBS
        pltpu.make_async_remote_copy(
            outer_ref.at[target],
            plane_ref.at[pl.ds(sub * 64, 64)],
            send.at[2],
            recv.at[2],
            device_id=(slab, target),
            device_id_type=MESH,
        ).start()
        return carry

    def pass_core(p, carry):
        target = (slab + NEAR + p // SUBS) % slabs
        pltpu.make_async_remote_copy(
            core_ref.at[pl.ds(p * 8, 8)],
            got_ref.at[pl.ds((p // SUBS * SUBS + sub) * 8, 8)],
            send.at[0],
            recv.at[0],
            device_id=(target, p % SUBS),
            device_id_type=MESH,
        ).start()
        return carry

    def pass_meta(d, carry):
        pltpu.make_async_remote_copy(
            meta_ref.at[pl.ds(0, 1)],
            told_ref.at[pl.ds(d, 1)],
            send.at[1],
            recv.at[1],
            device_id=((slab + NEAR + d) % slabs, sub),
            device_id_type=MESH,
        ).start()
        return carry

    lax.fori_loop(0, REACH, pass_meta, 0)
    lax.fori_loop(0, REACH * SUBS, pass_core, 0)
    lax.fori_loop(1, SUBS, pass_outer, 0)
    plane_ref[pl.ds(pl.multiple_of(sub * 64, 64), 64), :] = outer_ref[sub]
    for sem in (send, recv):
        wait_all(sem.at[0], got_ref)
        wait_all(sem.at[1], told_ref)
        wait_all(sem.at[2], plane_ref.at[pl.ds(0, 192)])


def forward_kernel(told_ref, got_ref, plane_ref, high_ref, low_ref, density_ref, spec_ref, wide, part):
    for half in range(2):
        wide[half, pl.ds(0, NX), :] = plane_ref[:, pl.ds(half * 128, 128)]
        wide[half, pl.ds(NX, CORE), :] = jnp.zeros((CORE, 128), f32)
    column = lanes((8, 128))

    def place(d, carry):
        base = pl.multiple_of(d * 32, 32)
        cells = got_ref[pl.ds(base, 8), :]
        for q in range(1, SUBS):
            cells = cells + got_ref[pl.ds(base + 8 * q, 8), :]
        start_x, start_y = told_ref[d, 0], told_ref[d, 1]
        for m in range(4):
            piece = pltpu.roll(cells, (128 - 32 * m) % 128, 1)
            piece = jnp.where(column < 32, piece, 0.0)
            piece = jnp.concatenate([piece, jnp.zeros((8, 128), f32)], axis=1)
            piece = pltpu.roll(piece, start_y, 1)
            part[0, pl.ds(m, 8, stride=4), :] = piece[:, :128]
            part[1, pl.ds(m, 8, stride=4), :] = piece[:, 128:]
        here = pl.ds(start_x, CORE)
        for half in range(2):
            wide[half, here, :] = wide[half, here, :] + part[half]
        return carry

    lax.fori_loop(0, REACH, place, 0)
    for half in range(2):
        again = wide[half, pl.ds(NX, CORE), :]
        wide[half, pl.ds(0, CORE), :] = wide[half, pl.ds(0, CORE), :] + again
    density = jnp.concatenate([wide[half, pl.ds(0, NX), :] for half in range(2)], axis=1)
    density_ref[...] = density
    table = (high_ref[...], low_ref[...])
    spec = dot3(table, split(dot3(split(density), table)))
    spec_ref[pl.ds(0, NX), :] = spec[:, :128]
    spec_ref[pl.ds(NX, NX), :] = spec[:, 128:]


def to_everyone(src, dst, me, count, send, recv):
    def one(i, carry):
        target = (me + i) % count
        pltpu.make_async_remote_copy(
            src.at[pl.ds(target, 1)],
            dst.at[pl.ds(me, 1)],
            send,
            recv,
            device_id=(target // SUBS, target % SUBS),
            device_id_type=MESH,
        ).start()
        return carry

    lax.fori_loop(1, count, one, 0)
    dst[pl.ds(me, 1), :] = src[pl.ds(me, 1), :]
    wait_all(recv, dst.at[pl.ds(0, count - 1)])


def wave_squares(index, count):
    folded = jnp.where(index > count // 2, index - count, index)
    wave = (2.0 * math.pi / (count * SPACING)) * folded.astype(f32)
    return wave * wave


def z_kernel(spec_ref, high_ref, low_ref, back_ref, got, turned, send, recv):
    count = lax.axis_size("slab") * SUBS
    me = lax.axis_index("slab") * SUBS + lax.axis_index("sub")
    to_everyone(spec_ref, got, me, count, send.at[0], recv.at[0])
    table = (high_ref[...], low_ref[...])
    values = dot3(table, split(got[...]))
    shape = (count, 128)
    square = (
        wave_squares(rows(shape), count)
        + wave_squares(jnp.zeros(shape, jnp.int32) + me % NX, NX)
        + wave_squares(lanes(shape) + me // NX * 128, NY)
    )
    factor = jnp.where(square > 0, 4.0 * math.pi / jnp.where(square > 0, square, 1.0), 0.0)
    turned[...] = dot3(table, split(values * factor))
    to_everyone(turned, back_ref, me, count, send.at[1], recv.at[1])
    for k in range(2):
        wait_all(send.at[k], back_ref.at[pl.ds(0, count - 1)])


def exchange_correlation(density):
    clipped = jnp.maximum(density, FLOOR)
    root = jnp.exp(jnp.log(clipped) * (1.0 / 3.0))
    radius = (3.0 / (4.0 * math.pi)) ** (1.0 / 3.0) / root
    exchange = -((3.0 / math.pi) ** (1.0 / 3.0)) * root
    inverse = 1.0 / (radius + 7.8)
    return exchange - 0.44 * inverse - (0.44 / 3.0) * radius * inverse * inverse


def inverse_kernel(corner_ref, back_ref, density_ref, high_ref, low_ref, potential_ref, window_ref, wide, cut):
    slab = lax.axis_index("slab")
    slabs = lax.axis_size("slab")
    table = (high_ref[...], low_ref[...])
    spec = jnp.concatenate([back_ref[pl.ds(0, NX), :], back_ref[pl.ds(NX, NX), :]], axis=1)
    hartree = dot3(split(dot3(table, split(spec))), table)
    potential = hartree + exchange_correlation(density_ref[...])
    potential_ref[...] = potential
    for half in range(2):
        side = potential[:, half * 128 : half * 128 + 128]
        wide[half, pl.ds(0, NX), :] = side
        wide[half, pl.ds(NX, BOX), :] = side[:BOX]

    def cut_one(k, carry):
        fragment = (slab - k // SUBS + slabs) % slabs * SUBS + k % SUBS
        start_x, start_y = corner_ref[fragment * 3 + 1], corner_ref[fragment * 3 + 2]
        here = pl.ds(start_x, BOX)
        strip = jnp.concatenate([wide[0, here, :], wide[1, here, :]], axis=1)
        strip = pltpu.roll(strip, (NY - start_y) % NY, 1)
        cut[pl.ds(pl.multiple_of(k * BOX, BOX), BOX), :] = strip[:, :128]
        return carry

    lax.fori_loop(0, SPREAD * SUBS, cut_one, 0)
    column = lanes((24, 128))

    def pack(k, carry):
        out = [jnp.zeros((24, 128), f32) for _ in range(3)]
        for b in range(8):
            tile, begin = b * BOX // 128, b * BOX % 128
            value = pltpu.roll(cut[pl.ds(k * 192 + b, 24, stride=8), :], begin, 1)
            here = (column >= begin) & (column < begin + BOX)
            out[tile] = jnp.where(here, value, out[tile])
            if begin + BOX > 128:
                out[tile + 1] = jnp.where(column < begin + BOX - 128, value, out[tile + 1])
        for t in range(3):
            window_ref[pl.ds(k * 72 + t, 24, stride=3), :] = out[t]
        return carry

    lax.fori_loop(0, SPREAD, pack, 0)


def gather_kernel(window_ref, potential_ref, frame_ref, out_ref, send, recv):
    slab, sub = lax.axis_index("slab"), lax.axis_index("sub")
    slabs = lax.axis_size("slab")

    def pass_window(k, carry):
        @pl.when(k != sub)
        def _():
            pltpu.make_async_remote_copy(
                window_ref.at[pl.ds(k * TILES, TILES)],
                frame_ref.at[pl.ds((k // SUBS * SUBS + sub) * TILES, TILES)],
                send.at[0],
                recv.at[0],
                device_id=((slab - k // SUBS + slabs) % slabs, k % SUBS),
                device_id_type=MESH,
            ).start()

        return carry

    def pass_plane(k, carry):
        target = (sub + k) % SUBS
        pltpu.make_async_remote_copy(
            potential_ref.at[pl.ds(target * 64, 64)],
            out_ref.at[sub],
            send.at[1],
            recv.at[1],
            device_id=(slab, target),
            device_id_type=MESH,
        ).start()
        return carry

    lax.fori_loop(0, SPREAD * SUBS, pass_window, 0)
    lax.fori_loop(1, SUBS, pass_plane, 0)
    frame_ref[pl.ds(sub * TILES, TILES), :] = window_ref[pl.ds(sub * TILES, TILES), :]
    out_ref[sub] = potential_ref[pl.ds(pl.multiple_of(sub * 64, 64), 64), :]
    for sem in (send, recv):
        wait_all(sem.at[0], frame_ref.at[pl.ds(0, (SPREAD * SUBS - 1) * TILES)])
        wait_all(sem.at[1], out_ref.at[pl.ds(0, SUBS - 1)])


def call(kernel, shapes, smem=0, count=0, scratch=(), remote=False, name=None):
    in_specs = [pl.BlockSpec(memory_space=pltpu.SMEM)] * smem + [
        pl.BlockSpec(memory_space=pltpu.VMEM)
    ] * (count - smem)
    return pl.pallas_call(
        kernel,
        out_shape=[jax.ShapeDtypeStruct(s, t) for s, t in shapes],
        in_specs=in_specs,
        out_specs=[pl.BlockSpec(memory_space=pltpu.VMEM)] * len(shapes),
        scratch_shapes=list(scratch),
        compiler_params=pltpu.CompilerParams(has_side_effects=remote),
        name=name,
    )


def body(orbitals, occupations, patch_sign, corners, core_span, outer_density):
    slab_id = lax.axis_index("slab")
    own = slab_id * SUBS + lax.axis_index("sub")
    count = lax.axis_size("slab") * SUBS
    flat_corners = corners.reshape(-1)
    weights = occupations[0].astype(f32) * patch_sign[0].astype(f32)
    box = jnp.sum(weights[:, None] * jnp.square(orbitals[0].astype(f32)), axis=0)
    sems = [pltpu.SemaphoreType.DMA((3,)), pltpu.SemaphoreType.DMA((3,))]
    core, meta = call(
        core_kernel, [((REACH * SUBS * 8, 128), f32), ((8, 128), jnp.int32)], 2, 3, name="core"
    )(core_span[0], flat_corners, box.reshape(BOX * TILES, 128))
    got, told, plane = call(
        spread_kernel,
        [((REACH * SUBS * 8, 128), f32), ((REACH, 128), jnp.int32), ((NX, NY), f32)],
        0,
        3,
        sems,
        True,
        name="spread",
    )(core, meta, outer_density)
    plane_table = [jnp.asarray(t) for t in cas_table(NX)]
    z_table = [jnp.asarray(t) for t in cas_table(count)]
    density, spec = call(
        forward_kernel,
        [((NX, NY), f32), ((count, 128), f32)],
        1,
        5,
        [pltpu.VMEM((2, NX + CORE, 128), f32), pltpu.VMEM((2, CORE, 128), f32)],
        name="forward",
    )(told, got, plane, *plane_table)
    (back,) = call(
        z_kernel,
        [((count, 128), f32)],
        0,
        3,
        [pltpu.VMEM((count, 128), f32), pltpu.VMEM((count, 128), f32), *sems],
        True,
        name="along_z",
    )(spec, *z_table)
    potential, windows = call(
        inverse_kernel,
        [((NX, NY), f32), ((SPREAD * SUBS * TILES, 128), f32)],
        1,
        5,
        [pltpu.VMEM((2, NX + BOX, 128), f32), pltpu.VMEM((SPREAD * SUBS * BOX, 128), f32)],
        name="inverse",
    )(flat_corners, back, density, *plane_table)
    frame, out = call(
        gather_kernel,
        [((SPREAD * SUBS * TILES, 128), f32), ((Z_DEV, NX // SUBS, NY), f32)],
        0,
        2,
        sems,
        True,
        name="gather",
    )(windows, potential)
    offset = corners[own, 0] - slab_id * Z_DEV
    planes = lax.dynamic_slice(frame, (offset * TILES, 0), (BOX * TILES, 128))
    return planes.reshape(1, BOX * BOX * BOX), out


def solution(mesh):
    placed = (
        P(("slab", "sub"), None, None),
        P(("slab", "sub"), None),
        P(("slab", "sub")),
        P(),
        P(("slab", "sub"), None),
        P("slab", "sub", None),
    )
    return jax.shard_map(
        body,
        mesh=mesh,
        in_specs=placed,
        out_specs=(P(("slab", "sub"), None), P("slab", "sub", None)),
        check_vma=False,
    )
```

```python
import math

import jax
import jax.numpy as jnp
import numpy as np
from jax import lax
from jax.experimental import pallas as pl
from jax.experimental.pallas import tpu as pltpu
from jax.sharding import PartitionSpec as P

BOX = 48
ORB = 16
NX = 256
NY = 256
Z_DEV = 4
SUBS = 4
CORE = 32
FIRST = 8
SPACING = 0.35
FLOOR = 0.001
NEAR = FIRST // Z_DEV
REACH = 11
SPREAD = 13
TILES = BOX * BOX // 128
MESH = pl.DeviceIdType.MESH
f32 = jnp.float32
bf16 = jnp.bfloat16


def cas_table(count):
    index = np.arange(count)
    angle = 2.0 * np.pi * ((index[:, None] * index[None, :]) % count) / count
    table = (np.cos(angle) + np.sin(angle)) / np.sqrt(count)
    high = table.astype(np.float32).astype(bf16)
    low = (table - high.astype(np.float64)).astype(np.float32).astype(bf16)
    return high, low


def split(values):
    high = values.astype(bf16)
    return high, (values - high.astype(f32)).astype(bf16)


def dot(a, b):
    return jnp.dot(a, b, preferred_element_type=f32)


def dot3(a, b):
    return dot(a[0], b[0]) + (dot(a[0], b[1]) + dot(a[1], b[0]))


def lanes(shape):
    return lax.broadcasted_iota(jnp.int32, shape, len(shape) - 1)


def rows(shape):
    return lax.broadcasted_iota(jnp.int32, shape, 0)


def wait_all(sem, ref):
    pltpu.make_async_copy(ref, ref, sem).wait()


def send(src, dst, send_sem, recv_sem, slab, sub):
    pltpu.make_async_remote_copy(
        src, dst, send_sem, recv_sem, device_id=(slab, sub), device_id_type=MESH
    ).start()


def far_first(j, count):
    return (count // 2 + (j + 1) // 2 * (1 - 2 * (j % 2))) % count


def partner(i, slab, sub, count):
    x, core, z, y = i % 4, i // 4 % 2, i // 8 % 8, i // 64
    zc = slab % 16
    target_z = (zc // 2 + far_first(z, 8)) % 8
    target_y = (slab // 16 + far_first(y, count // 64)) % (count // 64)
    target_core = (zc % 2 + 1 - core) % 2
    return (target_y * 8 + target_z) * 2 + target_core, (sub + far_first(x, 4)) % 4


def to_everyone(src, dst, slab, sub, count, send_sem, recv_sem):
    me = slab * SUBS + sub

    def one(i, carry):
        to_slab, to_sub = partner(i, slab, sub, count)
        send(
            src.at[pl.ds(to_slab * SUBS + to_sub, 1)],
            dst.at[pl.ds(me, 1)],
            send_sem,
            recv_sem,
            to_slab,
            to_sub,
        )
        return carry

    lax.fori_loop(0, count - 1, one, 0)
    dst[pl.ds(me, 1), :] = src[pl.ds(me, 1), :]
    wait_all(recv_sem, dst.at[pl.ds(0, count - 1)])


def wave_squares(index, count):
    folded = jnp.where(index > count // 2, index - count, index)
    wave = (2.0 * math.pi / (count * SPACING)) * folded.astype(f32)
    return wave * wave


def exchange_correlation(density):
    clipped = jnp.maximum(density, FLOOR)
    root = jnp.exp(jnp.log(clipped) * (1.0 / 3.0))
    radius = (3.0 / (4.0 * math.pi)) ** (1.0 / 3.0) / root
    exchange = -((3.0 / math.pi) ** (1.0 / 3.0)) * root
    inverse = 1.0 / (radius + 7.8)
    return exchange - 0.44 * inverse - (0.44 / 3.0) * radius * inverse * inverse


def density_rows(occupation_ref, sign_ref, orbital_ref, box):
    row = rows((ORB, 128))
    weight = jnp.zeros((ORB, 128), jnp.int32)
    for o in range(ORB):
        weight = jnp.where(row == o, occupation_ref[0, o] * sign_ref[0], weight)
    weight = weight.astype(f32)

    def one(g, carry):
        base = pl.multiple_of(g * 1024, 1024)
        values = orbital_ref[:, pl.ds(base, 1024)].astype(f32)
        out = pl.multiple_of(g * 8, 8)
        for j in range(8):
            part = values[:, j * 128 : j * 128 + 128]
            box[pl.ds(out + j, 1), :] = jnp.sum(weight * (part * part), axis=0, keepdims=True)
        return carry

    lax.fori_loop(FIRST * TILES // 8, BOX * TILES // 8, one, 0, unroll=2)


def core_planes(span_ref, corner_ref, box, staged, core, meta, slab, sub):
    own = slab * SUBS + sub
    first_z, first_x, first_y = span_ref[0, 0], span_ref[0, 1], span_ref[0, 2]
    long_z, long_x, long_y = span_ref[0, 3], span_ref[0, 4], span_ref[0, 5]
    offset = corner_ref[0, own] % Z_DEV
    planes = BOX - FIRST
    start = first_x * BOX + first_y
    tile, lane = start // 128, start % 128
    shape = (planes, 128)
    column = lanes(shape)
    turned = []
    for t in range(13):
        row = FIRST * TILES + jnp.minimum(tile + t, TILES - 1)
        raw = box[pl.ds(row, planes, stride=TILES), :]
        turned.append(pltpu.roll(raw, (128 - lane) % 128, 1))
    chunks = [jnp.where(column < 128 - lane, turned[t], turned[t + 1]) for t in range(12)]
    plane = rows(shape) + FIRST
    within_z = (plane >= first_z) & (plane < first_z + long_z)
    staged[pl.ds(0, 32), :] = jnp.zeros((32, 128), f32)
    staged[pl.ds(352, 32), :] = jnp.zeros((32, 128), f32)
    for t in range(8):
        value = jnp.zeros(shape, f32)
        for m in range(4):
            source = (4 * t + m) * BOX
            chunk, begin = source // 128, source % 128
            shift = (32 * m - begin) % 128
            piece = pltpu.roll(chunks[chunk], shift, 1)
            if begin + CORE > 128:
                after = pltpu.roll(chunks[chunk + 1], shift, 1)
                piece = jnp.where(column < 32 * m + 128 - begin, piece, after)
            value = jnp.where(column // 32 == m, piece, value)
        inside = within_z & (4 * t + column // 32 < long_x) & (column % 32 < long_y)
        staged[pl.ds(32 + t, planes, stride=8), :] = jnp.where(inside, value, 0.0)
    core[...] = staged[pl.ds((Z_DEV - offset) * 8, REACH * SUBS * 8), :]
    start_x = (corner_ref[1, own] + first_x) % NX
    start_y = (corner_ref[2, own] + first_y) % NY
    meta[...] = jnp.where(lanes((8, 128)) == 0, start_x, start_y)


def place_cores(first_cell, got, ring, wide):
    column = lanes((8, 128))
    ring[...] = jnp.zeros_like(ring)

    def place(d, carry):
        base = pl.multiple_of(d * 32, 32)
        cells = got[pl.ds(base, 8), :]
        for q in range(1, SUBS):
            cells = cells + got[pl.ds(base + 8 * q, 8), :]
        start_x, start_y = first_cell[d, 0], first_cell[d, 1]
        for m in range(4):
            piece = pltpu.roll(cells, (128 - 32 * m) % 128, 1)
            piece = jnp.where(column < 32, piece, 0.0)
            piece = jnp.concatenate([piece, jnp.zeros((8, 128), f32)], axis=1)
            piece = pltpu.roll(piece, start_y, 1)
            for half in range(2):
                side = piece[:, half * 128 : half * 128 + 128]
                ring[half, pl.ds(m, 8, stride=4), :] = side
                ring[half, pl.ds(NX + m, 8, stride=4), :] = side
        for half in range(2):
            wide[half, pl.ds(0, NX), :] = (
                wide[half, pl.ds(0, NX), :] + ring[half, pl.ds(NX - start_x, NX), :]
            )
        return carry

    lax.fori_loop(0, REACH, place, 0)


def whole_kernel(
    span_ref,
    corner_ref,
    occupation_ref,
    sign_ref,
    orbital_ref,
    outer_ref,
    high_ref,
    low_ref,
    high_z_ref,
    low_z_ref,
    box_out,
    grid_out,
    box,
    staged,
    core,
    meta,
    got,
    told,
    first_cell,
    outer,
    ring,
    wide,
    spec,
    got_z,
    turned,
    back,
    potential,
    cut,
    windows,
    frame,
    send_sem,
    recv_sem,
    local_sem,
):
    slab, sub = lax.axis_index("slab"), lax.axis_index("sub")
    slabs = lax.axis_size("slab")
    count = slabs * SUBS
    barrier = pltpu.get_barrier_semaphore()

    def greet(i, carry):
        pl.semaphore_signal(
            barrier, inc=1, device_id=partner(i, slab, sub, count), device_id_type=MESH
        )
        return carry

    lax.fori_loop(0, count - 1, greet, 0)
    density_rows(occupation_ref, sign_ref, orbital_ref, box)
    core_planes(span_ref, corner_ref, box, staged, core, meta, slab, sub)
    pl.semaphore_wait(barrier, count - 1)

    def pass_meta(j, carry):
        d = REACH - 1 - j
        to = (slab + NEAR + d) % slabs
        send(meta.at[pl.ds(0, 1)], told.at[pl.ds(d, 1)], send_sem.at[1], recv_sem.at[1], to, sub)
        return carry

    def pass_core(j, carry):
        p = REACH * SUBS - 1 - j
        src = core.at[pl.ds(p * 8, 8)]
        dst = got.at[pl.ds((p // SUBS * SUBS + sub) * 8, 8)]
        to = (slab + NEAR + p // SUBS) % slabs
        send(src, dst, send_sem.at[0], recv_sem.at[0], to, p % SUBS)
        return carry

    def pass_outer(k, carry):
        to = (sub + k) % SUBS
        dst = outer.at[pl.ds(sub * 64, 64)]
        send(outer_ref.at[to], dst, send_sem.at[2], recv_sem.at[2], slab, to)
        return carry

    lax.fori_loop(0, REACH, pass_meta, 0)
    lax.fori_loop(0, REACH * SUBS, pass_core, 0)
    lax.fori_loop(1, SUBS, pass_outer, 0)
    outer[pl.ds(pl.multiple_of(sub * 64, 64), 64), :] = outer_ref[sub]
    wait_all(recv_sem.at[2], outer.at[pl.ds(0, 192)])
    for half in range(2):
        wide[half, pl.ds(0, NX), :] = outer[:, pl.ds(half * 128, 128)]
    wait_all(recv_sem.at[1], told)
    tell = pltpu.make_async_copy(told, first_cell, local_sem)
    tell.start()
    tell.wait()
    wait_all(recv_sem.at[0], got)
    place_cores(first_cell, got, ring, wide)

    density = jnp.concatenate([wide[half, pl.ds(0, NX), :] for half in range(2)], axis=1)
    outer[...] = exchange_correlation(density)
    table = (high_ref[...], low_ref[...])
    values = dot3(table, split(dot3(split(density), table)))
    spec[pl.ds(0, NX), :] = values[:, :128]
    spec[pl.ds(NX, NX), :] = values[:, 128:]

    to_everyone(spec, got_z, slab, sub, count, send_sem.at[3], recv_sem.at[3])
    table_z = (high_z_ref[...], low_z_ref[...])
    values = dot3(table_z, split(got_z[...]))
    me = slab * SUBS + sub
    shape = (count, 128)
    square = (
        wave_squares(rows(shape), count)
        + wave_squares(jnp.zeros(shape, jnp.int32) + me % NX, NX)
        + wave_squares(lanes(shape) + me // NX * 128, NY)
    )
    factor = jnp.where(square > 0, 4.0 * math.pi / jnp.where(square > 0, square, 1.0), 0.0)
    turned[...] = dot3(table_z, split(values * factor))
    to_everyone(turned, back, slab, sub, count, send_sem.at[4], recv_sem.at[4])

    values = jnp.concatenate([back[pl.ds(0, NX), :], back[pl.ds(NX, NX), :]], axis=1)
    values = dot3(split(dot3(table, split(values))), table) + outer[...]
    potential[...] = values
    for half in range(2):
        side = values[:, half * 128 : half * 128 + 128]
        wide[half, pl.ds(0, NX), :] = side
        wide[half, pl.ds(NX, BOX), :] = side[:BOX]

    def pass_plane(k, carry):
        to = (sub + k) % SUBS
        src = potential.at[pl.ds(to * 64, 64)]
        send(src, grid_out.at[sub], send_sem.at[5], recv_sem.at[5], slab, to)
        return carry

    lax.fori_loop(1, SUBS, pass_plane, 0)

    column = lanes((24, 128))

    def windows_of(j, carry):
        d = jnp.where(j <= 8, 8 + (j + 1) // 2 * (1 - 2 * (j % 2)), SPREAD - 1 - j)
        to = (slab - d + slabs) % slabs
        for q in range(SUBS):
            fragment = to * SUBS + q
            start_x, start_y = corner_ref[1, fragment], corner_ref[2, fragment]
            here = pl.ds(start_x, BOX)
            strip = jnp.concatenate([wide[0, here, :], wide[1, here, :]], axis=1)
            strip = pltpu.roll(strip, (NY - start_y) % NY, 1)
            cut[pl.ds(q * BOX, BOX), :] = strip[:, :128]
        out = [jnp.zeros((24, 128), f32) for _ in range(3)]
        for b in range(8):
            tile, begin = b * BOX // 128, b * BOX % 128
            value = pltpu.roll(cut[pl.ds(b, 24, stride=8), :], begin, 1)
            here = (column >= begin) & (column < begin + BOX)
            out[tile] = jnp.where(here, value, out[tile])
            if begin + BOX > 128:
                out[tile + 1] = jnp.where(column < begin + BOX - 128, value, out[tile + 1])
        for t in range(3):
            windows[pl.ds(d * 72 + t, 24, stride=3), :] = out[t]

        def pass_window(q, carry):
            @pl.when((d > 0) | (q != sub))
            def _():
                src = windows.at[pl.ds((d * SUBS + q) * TILES, TILES)]
                dst = frame.at[pl.ds((d * SUBS + sub) * TILES, TILES)]
                send(src, dst, send_sem.at[6], recv_sem.at[6], to, q)

            return carry

        return lax.fori_loop(0, SUBS, pass_window, carry)

    lax.fori_loop(0, SPREAD, windows_of, 0)
    frame[pl.ds(sub * TILES, TILES), :] = windows[pl.ds(sub * TILES, TILES), :]
    grid_out[sub] = potential[pl.ds(pl.multiple_of(sub * 64, 64), 64), :]
    own_windows = frame.at[pl.ds(0, (SPREAD * SUBS - 1) * TILES)]
    wait_all(recv_sem.at[6], own_windows)
    offset = corner_ref[0, me] % Z_DEV
    box_out[...] = frame[pl.ds(offset * TILES, BOX * TILES), :]
    wait_all(recv_sem.at[5], grid_out.at[pl.ds(0, SUBS - 1)])
    wait_all(send_sem.at[0], got)
    wait_all(send_sem.at[1], told)
    wait_all(send_sem.at[2], outer.at[pl.ds(0, 192)])
    wait_all(send_sem.at[3], back.at[pl.ds(0, count - 1)])
    wait_all(send_sem.at[4], back.at[pl.ds(0, count - 1)])
    wait_all(send_sem.at[5], grid_out.at[pl.ds(0, SUBS - 1)])
    wait_all(send_sem.at[6], own_windows)


def body(orbitals, occupations, patch_sign, corners, core_span, outer_density):
    count = lax.axis_size("slab") * SUBS
    tables = [jnp.asarray(t) for t in (*cas_table(NX), *cas_table(count))]
    smem = pl.BlockSpec(memory_space=pltpu.SMEM)
    vmem = pl.BlockSpec(memory_space=pltpu.VMEM)
    cores = (REACH * SUBS * 8, 128)
    planes = (SPREAD * SUBS * TILES, 128)
    box_potential, potential = pl.pallas_call(
        whole_kernel,
        out_shape=[
            jax.ShapeDtypeStruct((BOX * TILES, 128), f32),
            jax.ShapeDtypeStruct((Z_DEV, NX // SUBS, NY), f32),
        ],
        in_specs=[smem] * 4 + [vmem] * 6,
        out_specs=[vmem] * 2,
        scratch_shapes=[
            pltpu.VMEM((BOX * TILES, 128), f32),
            pltpu.VMEM((384, 128), f32),
            pltpu.VMEM(cores, f32),
            pltpu.VMEM((8, 128), jnp.int32),
            pltpu.VMEM(cores, f32),
            pltpu.VMEM((REACH, 128), jnp.int32),
            pltpu.SMEM((REACH, 128), jnp.int32),
            pltpu.VMEM((NX, NY), f32),
            pltpu.VMEM((2, 2 * NX, 128), f32),
            pltpu.VMEM((2, NX + BOX, 128), f32),
            pltpu.VMEM((count, 128), f32),
            pltpu.VMEM((count, 128), f32),
            pltpu.VMEM((count, 128), f32),
            pltpu.VMEM((count, 128), f32),
            pltpu.VMEM((NX, NY), f32),
            pltpu.VMEM((SUBS * BOX, 128), f32),
            pltpu.VMEM(planes, f32),
            pltpu.VMEM(planes, f32),
            pltpu.SemaphoreType.DMA((7,)),
            pltpu.SemaphoreType.DMA((7,)),
            pltpu.SemaphoreType.DMA,
        ],
        compiler_params=pltpu.CompilerParams(collective_id=0, has_side_effects=True),
        name="whole",
    )(core_span, corners.T, occupations, patch_sign, orbitals[0], outer_density, *tables)
    return box_potential.reshape(1, BOX * BOX * BOX), potential


def solution(mesh):
    placed = (
        P(("slab", "sub"), None, None),
        P(("slab", "sub"), None),
        P(("slab", "sub")),
        P(),
        P(("slab", "sub"), None),
        P("slab", "sub", None),
    )
    return jax.shard_map(
        body,
        mesh=mesh,
        in_specs=placed,
        out_specs=(P(("slab", "sub"), None), P("slab", "sub", None)),
        check_vma=False,
    )
```

```python
import math

import jax
import jax.numpy as jnp
import numpy as np
from jax import lax
from jax.experimental import pallas as pl
from jax.experimental.pallas import tpu as pltpu
from jax.sharding import PartitionSpec as P

BOX = 48
ORB = 16
NX = 256
NY = 256
Z_DEV = 4
SUBS = 4
CORE = 32
FIRST = 8
SPACING = 0.35
FLOOR = 0.001
NEAR = FIRST // Z_DEV
REACH = 11
SPREAD = 13
TILES = BOX * BOX // 128
MESH = pl.DeviceIdType.MESH
f32 = jnp.float32
bf16 = jnp.bfloat16


def cas_table(count):
    index = np.arange(count)
    angle = 2.0 * np.pi * ((index[:, None] * index[None, :]) % count) / count
    table = (np.cos(angle) + np.sin(angle)) / np.sqrt(count)
    high = table.astype(np.float32).astype(bf16)
    low = (table - high.astype(np.float64)).astype(np.float32).astype(bf16)
    return high, low


def split(values):
    high = values.astype(bf16)
    return high, (values - high.astype(f32)).astype(bf16)


def dot(a, b):
    return jnp.dot(a, b, preferred_element_type=f32)


def dot3(a, b):
    return dot(a[0], b[0]) + (dot(a[0], b[1]) + dot(a[1], b[0]))


def lanes(shape):
    return lax.broadcasted_iota(jnp.int32, shape, len(shape) - 1)


def rows(shape):
    return lax.broadcasted_iota(jnp.int32, shape, 0)


def wait_all(sem, ref):
    pltpu.make_async_copy(ref, ref, sem).wait()


def send(src, dst, send_sem, recv_sem, slab, sub):
    pltpu.make_async_remote_copy(
        src, dst, send_sem, recv_sem, device_id=(slab, sub), device_id_type=MESH
    ).start()


def for_all_others(slab, sub, slabs, visit):
    subs = [sub] + [lax.rem(sub + k, SUBS) for k in range(1, SUBS)]
    line = 16
    lines = slabs // line
    here, row = lax.rem(slab, line), lax.div(slab, line)
    steps = sorted(range(lines), key=lambda k: -min(k, lines - k))
    for step in steps:
        base = lax.rem(row + step, lines) * line

        def one(i, carry):
            target = base + lax.rem(here + i, line)
            for k in (2, 1, 3, 0):
                visit(target, subs[k])
            return carry

        lax.fori_loop(0 if step else 1, line, one, 0)
    for k in range(1, SUBS):
        visit(slab, subs[k])


def to_everyone(src, dst, slab, sub, slabs, send_sem, recv_sem):
    here = pl.ds(slab * SUBS + sub, 1)

    def visit(to_slab, to_sub):
        row = pl.ds(to_slab * SUBS + to_sub, 1)
        send(src.at[row], dst.at[here], send_sem, recv_sem, to_slab, to_sub)

    for_all_others(slab, sub, slabs, visit)
    dst[here, :] = src[here, :]


def wave_squares(index, count):
    folded = jnp.where(index > count // 2, index - count, index)
    wave = (2.0 * math.pi / (count * SPACING)) * folded.astype(f32)
    return wave * wave


def exchange_correlation(density):
    clipped = jnp.maximum(density, FLOOR)
    root = jnp.exp(jnp.log(clipped) * (1.0 / 3.0))
    radius = (3.0 / (4.0 * math.pi)) ** (1.0 / 3.0) / root
    exchange = -((3.0 / math.pi) ** (1.0 / 3.0)) * root
    inverse = 1.0 / (radius + 7.8)
    return exchange - 0.44 * inverse - (0.44 / 3.0) * radius * inverse * inverse


def density_rows(occupation_ref, sign_ref, orbital_ref, box):
    row = rows((ORB, 128))
    weight = jnp.zeros((ORB, 128), jnp.int32)
    for o in range(ORB):
        weight = jnp.where(row == o, occupation_ref[0, o] * sign_ref[0], weight)
    weight = weight.astype(f32)

    def one(g, carry):
        base = pl.multiple_of(g * 1024, 1024)
        values = orbital_ref[:, pl.ds(base, 1024)].astype(f32)
        out = pl.multiple_of(g * 8, 8)
        for j in range(8):
            part = values[:, j * 128 : j * 128 + 128]
            box[pl.ds(out + j, 1), :] = jnp.sum(weight * (part * part), axis=0, keepdims=True)
        return carry

    lax.fori_loop(FIRST * TILES // 8, BOX * TILES // 8, one, 0, unroll=2)


def core_planes(span_ref, corner_ref, box, staged, core, meta, slab, sub):
    own = slab * SUBS + sub
    first_z, first_x, first_y = span_ref[0, 0], span_ref[0, 1], span_ref[0, 2]
    long_z, long_x, long_y = span_ref[0, 3], span_ref[0, 4], span_ref[0, 5]
    offset = corner_ref[0, own] % Z_DEV
    planes = BOX - FIRST
    start = first_x * BOX + first_y
    tile, lane = start // 128, start % 128
    shape = (planes, 128)
    column = lanes(shape)
    turned = []
    for t in range(13):
        row = FIRST * TILES + jnp.minimum(tile + t, TILES - 1)
        raw = box[pl.ds(row, planes, stride=TILES), :]
        turned.append(pltpu.roll(raw, (128 - lane) % 128, 1))
    chunks = [jnp.where(column < 128 - lane, turned[t], turned[t + 1]) for t in range(12)]
    plane = rows(shape) + FIRST
    within_z = (plane >= first_z) & (plane < first_z + long_z)
    staged[pl.ds(0, 32), :] = jnp.zeros((32, 128), f32)
    staged[pl.ds(352, 32), :] = jnp.zeros((32, 128), f32)
    for t in range(8):
        value = jnp.zeros(shape, f32)
        for m in range(4):
            source = (4 * t + m) * BOX
            chunk, begin = source // 128, source % 128
            shift = (32 * m - begin) % 128
            piece = pltpu.roll(chunks[chunk], shift, 1)
            if begin + CORE > 128:
                after = pltpu.roll(chunks[chunk + 1], shift, 1)
                piece = jnp.where(column < 32 * m + 128 - begin, piece, after)
            value = jnp.where(column // 32 == m, piece, value)
        inside = within_z & (4 * t + column // 32 < long_x) & (column % 32 < long_y)
        staged[pl.ds(32 + t, planes, stride=8), :] = jnp.where(inside, value, 0.0)
    core[...] = staged[pl.ds((Z_DEV - offset) * 8, REACH * SUBS * 8), :]
    start_x = (corner_ref[1, own] + first_x) % NX
    start_y = (corner_ref[2, own] + first_y) % NY
    meta[...] = jnp.where(lanes((8, 128)) == 0, start_x, start_y)


def place_cores(first_cell, got, ring, wide):
    column = lanes((8, 128))
    ring[...] = jnp.zeros_like(ring)

    def place(d, carry):
        base = pl.multiple_of(d * 32, 32)
        cells = got[pl.ds(base, 8), :]
        for q in range(1, SUBS):
            cells = cells + got[pl.ds(base + 8 * q, 8), :]
        start_x, start_y = first_cell[d, 0], first_cell[d, 1]
        for m in range(4):
            piece = pltpu.roll(cells, (128 - 32 * m) % 128, 1)
            piece = jnp.where(column < 32, piece, 0.0)
            piece = jnp.concatenate([piece, jnp.zeros((8, 128), f32)], axis=1)
            piece = pltpu.roll(piece, start_y, 1)
            for half in range(2):
                side = piece[:, half * 128 : half * 128 + 128]
                ring[half, pl.ds(m, 8, stride=4), :] = side
                ring[half, pl.ds(NX + m, 8, stride=4), :] = side
        for half in range(2):
            wide[half, pl.ds(0, NX), :] = (
                wide[half, pl.ds(0, NX), :] + ring[half, pl.ds(NX - start_x, NX), :]
            )
        return carry

    lax.fori_loop(0, REACH, place, 0)


def whole_kernel(
    span_ref,
    corner_ref,
    occupation_ref,
    sign_ref,
    orbital_ref,
    outer_ref,
    high_ref,
    low_ref,
    high_z_ref,
    low_z_ref,
    box_out,
    grid_out,
    box,
    staged,
    core,
    meta,
    got,
    told,
    first_cell,
    outer,
    ring,
    wide,
    spec,
    got_z,
    turned,
    back,
    potential,
    cut,
    windows,
    frame,
    send_sem,
    recv_sem,
    local_sem,
    orbitals,
    high,
    low,
    high_z,
    low_z,
):
    slab, sub = lax.axis_index("slab"), lax.axis_index("sub")
    slabs = lax.axis_size("slab")
    count = slabs * SUBS
    barrier = pltpu.get_barrier_semaphore()

    loads = [
        pltpu.make_async_copy(orbital_ref, orbitals, local_sem.at[0]),
        pltpu.make_async_copy(high_ref, high, local_sem.at[1]),
        pltpu.make_async_copy(low_ref, low, local_sem.at[2]),
        pltpu.make_async_copy(high_z_ref, high_z, local_sem.at[3]),
        pltpu.make_async_copy(low_z_ref, low_z, local_sem.at[4]),
        pltpu.make_async_copy(outer_ref.at[sub], outer.at[pl.ds(sub * 64, 64)], local_sem.at[5]),
    ]
    for load in loads:
        load.start()

    def greet(to_slab, to_sub):
        pl.semaphore_signal(barrier, inc=1, device_id=(to_slab, to_sub), device_id_type=MESH)

    for_all_others(slab, sub, slabs, greet)
    loads[0].wait()
    density_rows(occupation_ref, sign_ref, orbitals, box)
    core_planes(span_ref, corner_ref, box, staged, core, meta, slab, sub)
    pl.semaphore_wait(barrier, count - 1)

    def pass_cores(j, carry):
        d = REACH - 1 - j
        to = lax.rem(slab + NEAR + d, slabs)
        send(meta.at[pl.ds(0, 1)], told.at[pl.ds(d, 1)], send_sem.at[1], recv_sem.at[1], to, sub)
        for q in range(SUBS):
            src = core.at[pl.ds((d * SUBS + q) * 8, 8)]
            dst = got.at[pl.ds((d * SUBS + sub) * 8, 8)]
            send(src, dst, send_sem.at[0], recv_sem.at[0], to, q)
        return carry

    def pass_outer(k, carry):
        to = lax.rem(sub + k, SUBS)
        dst = outer.at[pl.ds(sub * 64, 64)]
        send(outer_ref.at[to], dst, send_sem.at[2], recv_sem.at[2], slab, to)
        return carry

    lax.fori_loop(0, REACH, pass_cores, 0)
    lax.fori_loop(1, SUBS, pass_outer, 0)
    for load in loads[1:]:
        load.wait()
    wait_all(recv_sem.at[2], outer.at[pl.ds(0, 192)])
    for half in range(2):
        wide[half, pl.ds(0, NX), :] = outer[:, pl.ds(half * 128, 128)]
    wait_all(recv_sem.at[1], told)
    tell = pltpu.make_async_copy(told, first_cell, local_sem.at[6])
    tell.start()
    tell.wait()
    wait_all(recv_sem.at[0], got)
    place_cores(first_cell, got, ring, wide)

    density = jnp.concatenate([wide[half, pl.ds(0, NX), :] for half in range(2)], axis=1)
    table = (high[...], low[...])
    values = dot3(table, split(dot3(split(density), table)))
    spec[pl.ds(0, NX), :] = values[:, :128]
    spec[pl.ds(NX, NX), :] = values[:, 128:]

    to_everyone(spec, got_z, slab, sub, slabs, send_sem.at[3], recv_sem.at[3])
    outer[...] = exchange_correlation(density)
    me = slab * SUBS + sub
    shape = (count, 128)
    square = (
        wave_squares(rows(shape), count)
        + wave_squares(jnp.zeros(shape, jnp.int32) + lax.rem(me, NX), NX)
        + wave_squares(lanes(shape) + lax.div(me, NX) * 128, NY)
    )
    turned[...] = jnp.where(square > 0, 4.0 * math.pi / jnp.where(square > 0, square, 1.0), 0.0)
    wait_all(recv_sem.at[3], got_z.at[pl.ds(0, count - 1)])
    table_z = (high_z[...], low_z[...])
    values = dot3(table_z, split(got_z[...])) * turned[...]
    turned[...] = dot3(table_z, split(values))
    to_everyone(turned, back, slab, sub, slabs, send_sem.at[4], recv_sem.at[4])
    wait_all(recv_sem.at[4], back.at[pl.ds(0, count - 1)])

    values = jnp.concatenate([back[pl.ds(0, NX), :], back[pl.ds(NX, NX), :]], axis=1)
    values = dot3(split(dot3(table, split(values))), table) + outer[...]
    potential[...] = values
    for half in range(2):
        side = values[:, half * 128 : half * 128 + 128]
        wide[half, pl.ds(0, NX), :] = side
        wide[half, pl.ds(NX, BOX), :] = side[:BOX]

    def pass_plane(k, carry):
        to = lax.rem(sub + k, SUBS)
        src = potential.at[pl.ds(to * 64, 64)]
        send(src, grid_out.at[sub], send_sem.at[5], recv_sem.at[5], slab, to)
        return carry

    lax.fori_loop(1, SUBS, pass_plane, 0)

    column = lanes((24, 128))

    def windows_of(j, carry):
        swing = lax.div(j + 1, 2) * (1 - 2 * lax.rem(j, 2))
        d = jnp.where(j <= 8, 8 + swing, SPREAD - 1 - j)
        to = lax.rem(slab - d + slabs, slabs)
        for q in range(SUBS):
            fragment = to * SUBS + q
            start_x, start_y = corner_ref[1, fragment], corner_ref[2, fragment]
            here = pl.ds(start_x, BOX)
            strip = jnp.concatenate([wide[0, here, :], wide[1, here, :]], axis=1)
            strip = pltpu.roll(strip, (NY - start_y) % NY, 1)
            cut[pl.ds(q * BOX, BOX), :] = strip[:, :128]
        out = [jnp.zeros((24, 128), f32) for _ in range(3)]
        for b in range(8):
            tile, begin = b * BOX // 128, b * BOX % 128
            value = pltpu.roll(cut[pl.ds(b, 24, stride=8), :], begin, 1)
            here = (column >= begin) & (column < begin + BOX)
            out[tile] = jnp.where(here, value, out[tile])
            if begin + BOX > 128:
                out[tile + 1] = jnp.where(column < begin + BOX - 128, value, out[tile + 1])
        for t in range(3):
            windows[pl.ds(d * 72 + t, 24, stride=3), :] = out[t]

        for q in range(SUBS):
            src = windows.at[pl.ds((d * SUBS + q) * TILES, TILES)]
            dst = frame.at[pl.ds((d * SUBS + sub) * TILES, TILES)]

            @pl.when((d > 0) | (sub != q))
            def _():
                send(src, dst, send_sem.at[6], recv_sem.at[6], to, q)

        return carry

    lax.fori_loop(0, SPREAD, windows_of, 0)
    frame[pl.ds(sub * TILES, TILES), :] = windows[pl.ds(sub * TILES, TILES), :]
    grid_out[sub] = potential[pl.ds(pl.multiple_of(sub * 64, 64), 64), :]
    own_windows = frame.at[pl.ds(0, (SPREAD * SUBS - 1) * TILES)]
    wait_all(recv_sem.at[6], own_windows)
    offset = corner_ref[0, me] % Z_DEV
    box_out[...] = frame[pl.ds(offset * TILES, BOX * TILES), :]
    wait_all(recv_sem.at[5], grid_out.at[pl.ds(0, SUBS - 1)])
    wait_all(send_sem.at[0], got)
    wait_all(send_sem.at[1], told)
    wait_all(send_sem.at[2], outer.at[pl.ds(0, 192)])
    wait_all(send_sem.at[3], back.at[pl.ds(0, count - 1)])
    wait_all(send_sem.at[4], back.at[pl.ds(0, count - 1)])
    wait_all(send_sem.at[5], grid_out.at[pl.ds(0, SUBS - 1)])
    wait_all(send_sem.at[6], own_windows)


def body(orbitals, occupations, patch_sign, corners, core_span, outer_density):
    count = lax.axis_size("slab") * SUBS
    tables = [jnp.asarray(t) for t in (*cas_table(NX), *cas_table(count))]
    smem = pl.BlockSpec(memory_space=pltpu.SMEM)
    vmem = pl.BlockSpec(memory_space=pltpu.VMEM)
    cores = (REACH * SUBS * 8, 128)
    planes = (SPREAD * SUBS * TILES, 128)
    box_potential, potential = pl.pallas_call(
        whole_kernel,
        out_shape=[
            jax.ShapeDtypeStruct((BOX * TILES, 128), f32),
            jax.ShapeDtypeStruct((Z_DEV, NX // SUBS, NY), f32),
        ],
        in_specs=[smem] * 4 + [pl.BlockSpec(memory_space=pl.ANY)] * 6,
        out_specs=[vmem] * 2,
        scratch_shapes=[
            pltpu.VMEM((BOX * TILES, 128), f32),
            pltpu.VMEM((384, 128), f32),
            pltpu.VMEM(cores, f32),
            pltpu.VMEM((8, 128), jnp.int32),
            pltpu.VMEM(cores, f32),
            pltpu.VMEM((REACH, 128), jnp.int32),
            pltpu.SMEM((REACH, 128), jnp.int32),
            pltpu.VMEM((NX, NY), f32),
            pltpu.VMEM((2, 2 * NX, 128), f32),
            pltpu.VMEM((2, NX + BOX, 128), f32),
            pltpu.VMEM((count, 128), f32),
            pltpu.VMEM((count, 128), f32),
            pltpu.VMEM((count, 128), f32),
            pltpu.VMEM((count, 128), f32),
            pltpu.VMEM((NX, NY), f32),
            pltpu.VMEM((SUBS * BOX, 128), f32),
            pltpu.VMEM(planes, f32),
            pltpu.VMEM(planes, f32),
            pltpu.SemaphoreType.DMA((7,)),
            pltpu.SemaphoreType.DMA((7,)),
            pltpu.SemaphoreType.DMA((7,)),
            pltpu.VMEM((ORB, BOX * BOX * BOX), bf16),
            pltpu.VMEM((NX, NY), bf16),
            pltpu.VMEM((NX, NY), bf16),
            pltpu.VMEM((count, count), bf16),
            pltpu.VMEM((count, count), bf16),
        ],
        compiler_params=pltpu.CompilerParams(collective_id=0, has_side_effects=True),
        name="whole",
    )(core_span, corners.T, occupations, patch_sign, orbitals[0], outer_density, *tables)
    return box_potential.reshape(1, BOX * BOX * BOX), potential


def solution(mesh):
    placed = (
        P(("slab", "sub"), None, None),
        P(("slab", "sub"), None),
        P(("slab", "sub")),
        P(),
        P(("slab", "sub"), None),
        P("slab", "sub", None),
    )
    return jax.shard_map(
        body,
        mesh=mesh,
        in_specs=placed,
        out_specs=(P(("slab", "sub"), None), P("slab", "sub", None)),
        check_vma=False,
    )
```

```python
import math

import jax
import jax.numpy as jnp
import numpy as np
from jax import lax
from jax.experimental import pallas as pl
from jax.experimental.pallas import tpu as pltpu
from jax.sharding import PartitionSpec as P

BOX = 48
ORB = 16
NX = 256
NY = 256
Z_DEV = 4
SUBS = 4
LINE = 16
CORE = 32
FIRST = 8
SPACING = 0.35
FLOOR = 0.001
NEAR = FIRST // Z_DEV
REACH = 11
SPREAD = 13
TILES = BOX * BOX // 128
MESH = pl.DeviceIdType.MESH
f32 = jnp.float32
bf16 = jnp.bfloat16


def cas_table(count):
    index = np.arange(count)
    angle = 2.0 * np.pi * ((index[:, None] * index[None, :]) % count) / count
    table = (np.cos(angle) + np.sin(angle)) / np.sqrt(count)
    high = table.astype(np.float32).astype(bf16)
    low = (table - high.astype(np.float64)).astype(np.float32).astype(bf16)
    return high, low


def split(values):
    high = values.astype(bf16)
    return high, (values - high.astype(f32)).astype(bf16)


def dot(a, b):
    return jnp.dot(a, b, preferred_element_type=f32)


def dot3(a, b):
    return dot(a[0], b[0]) + (dot(a[0], b[1]) + dot(a[1], b[0]))


def lanes(shape):
    return lax.broadcasted_iota(jnp.int32, shape, len(shape) - 1)


def rows(shape):
    return lax.broadcasted_iota(jnp.int32, shape, 0)


def wait_all(sem, ref):
    pltpu.make_async_copy(ref, ref, sem).wait()


def send(src, dst, send_sem, recv_sem, slab, sub):
    pltpu.make_async_remote_copy(
        src, dst, send_sem, recv_sem, device_id=(slab, sub), device_id_type=MESH
    ).start()


def for_all_others(slab, sub, slabs, visit):
    subs = [sub] + [lax.rem(sub + k, SUBS) for k in range(1, SUBS)]
    lines = slabs // LINE
    here, row = lax.rem(slab, LINE), lax.div(slab, LINE)
    steps = sorted(range(lines), key=lambda k: -min(k, lines - k))
    for step in steps:
        base = lax.rem(row + step, lines) * LINE

        def one(i, carry):
            target = base + lax.rem(here + i, LINE)
            for k in (2, 1, 3, 0):
                visit(target, subs[k])
            return carry

        lax.fori_loop(0 if step else 1, LINE, one, 0)
    for k in range(1, SUBS):
        visit(slab, subs[k])


def to_everyone(src, dst, slab, sub, slabs, send_sem, recv_sem):
    here = pl.ds(slab * SUBS + sub, 1)

    def visit(to_slab, to_sub):
        row = pl.ds(to_slab * SUBS + to_sub, 1)
        send(src.at[row], dst.at[here], send_sem, recv_sem, to_slab, to_sub)

    for_all_others(slab, sub, slabs, visit)
    dst[here, :] = src[here, :]


def wave_squares(index, count):
    folded = jnp.where(index > count // 2, index - count, index)
    wave = (2.0 * math.pi / (count * SPACING)) * folded.astype(f32)
    return wave * wave


def exchange_correlation(density):
    clipped = jnp.maximum(density, FLOOR)
    root = jnp.exp(jnp.log(clipped) * (1.0 / 3.0))
    radius = (3.0 / (4.0 * math.pi)) ** (1.0 / 3.0) / root
    exchange = -((3.0 / math.pi) ** (1.0 / 3.0)) * root
    inverse = 1.0 / (radius + 7.8)
    return exchange - 0.44 * inverse - (0.44 / 3.0) * radius * inverse * inverse


def density_rows(occupation_ref, sign_ref, orbital_ref, box):
    row = rows((ORB, 128))
    weight = jnp.zeros((ORB, 128), jnp.int32)
    for o in range(ORB):
        weight = jnp.where(row == o, occupation_ref[0, o] * sign_ref[0, 0], weight)
    weight = weight.astype(f32)

    def one(g, carry):
        base = pl.multiple_of(g * 1024, 1024)
        values = orbital_ref[:, pl.ds(base, 1024)].astype(f32)
        out = pl.multiple_of(g * 8, 8)
        for j in range(8):
            part = values[:, j * 128 : j * 128 + 128]
            box[pl.ds(out + j, 1), :] = jnp.sum(weight * (part * part), axis=0, keepdims=True)
        return carry

    lax.fori_loop(FIRST * TILES // 8, BOX * TILES // 8, one, 0, unroll=2)


def core_planes(span_ref, corner_ref, box, staged, core, meta, slab, sub):
    own = slab * SUBS + sub
    first_z, first_x, first_y = span_ref[0, 0], span_ref[0, 1], span_ref[0, 2]
    long_z, long_x, long_y = span_ref[0, 3], span_ref[0, 4], span_ref[0, 5]
    offset = corner_ref[0, own] % Z_DEV
    planes = BOX - FIRST
    start = first_x * BOX + first_y
    tile, lane = start // 128, start % 128
    shape = (planes, 128)
    column = lanes(shape)
    turned = []
    for t in range(13):
        row = FIRST * TILES + jnp.minimum(tile + t, TILES - 1)
        raw = box[pl.ds(row, planes, stride=TILES), :]
        turned.append(pltpu.roll(raw, (128 - lane) % 128, 1))
    chunks = [jnp.where(column < 128 - lane, turned[t], turned[t + 1]) for t in range(12)]
    plane = rows(shape) + FIRST
    within_z = (plane >= first_z) & (plane < first_z + long_z)
    staged[pl.ds(0, 32), :] = jnp.zeros((32, 128), f32)
    staged[pl.ds(352, 32), :] = jnp.zeros((32, 128), f32)
    for t in range(8):
        value = jnp.zeros(shape, f32)
        for m in range(4):
            source = (4 * t + m) * BOX
            chunk, begin = source // 128, source % 128
            shift = (32 * m - begin) % 128
            piece = pltpu.roll(chunks[chunk], shift, 1)
            if begin + CORE > 128:
                after = pltpu.roll(chunks[chunk + 1], shift, 1)
                piece = jnp.where(column < 32 * m + 128 - begin, piece, after)
            value = jnp.where(column // 32 == m, piece, value)
        inside = within_z & (4 * t + column // 32 < long_x) & (column % 32 < long_y)
        staged[pl.ds(32 + t, planes, stride=8), :] = jnp.where(inside, value, 0.0)
    core[...] = staged[pl.ds((Z_DEV - offset) * 8, REACH * SUBS * 8), :]
    start_x = (corner_ref[1, own] + first_x) % NX
    start_y = (corner_ref[2, own] + first_y) % NY
    meta[...] = jnp.where(lanes((8, 128)) == 0, start_x, start_y)


def place_cores(first_cell, got, ring, wide):
    column = lanes((8, 128))
    ring[...] = jnp.zeros_like(ring)

    def place(d, carry):
        base = pl.multiple_of(d * 32, 32)
        cells = got[pl.ds(base, 8), :]
        for q in range(1, SUBS):
            cells = cells + got[pl.ds(base + 8 * q, 8), :]
        start_x, start_y = first_cell[d, 0], first_cell[d, 1]
        for m in range(4):
            piece = pltpu.roll(cells, (128 - 32 * m) % 128, 1)
            piece = jnp.where(column < 32, piece, 0.0)
            piece = jnp.concatenate([piece, jnp.zeros((8, 128), f32)], axis=1)
            piece = pltpu.roll(piece, start_y, 1)
            for half in range(2):
                side = piece[:, half * 128 : half * 128 + 128]
                ring[half, pl.ds(m, 8, stride=4), :] = side
                ring[half, pl.ds(NX + m, 8, stride=4), :] = side
        for half in range(2):
            wide[half, pl.ds(0, NX), :] = (
                wide[half, pl.ds(0, NX), :] + ring[half, pl.ds(NX - start_x, NX), :]
            )
        return carry

    lax.fori_loop(0, REACH, place, 0)


def whole_kernel(
    span_ref,
    corner_ref,
    occupation_ref,
    sign_ref,
    orbital_ref,
    outer_ref,
    high_ref,
    low_ref,
    high_z_ref,
    low_z_ref,
    frame,
    grid_out,
    box,
    staged,
    core,
    meta,
    got,
    told,
    first_cell,
    outer,
    ring,
    wide,
    spec,
    got_z,
    turned,
    back,
    potential,
    cut,
    windows,
    send_sem,
    recv_sem,
    local_sem,
    column_sem,
    orbitals,
    high,
    low,
    high_z,
    low_z,
):
    slab, sub = lax.axis_index("slab"), lax.axis_index("sub")
    slabs = lax.axis_size("slab")
    count = slabs * SUBS
    barrier = pltpu.get_barrier_semaphore()

    loads = [
        pltpu.make_async_copy(orbital_ref, orbitals, local_sem.at[0]),
        pltpu.make_async_copy(high_ref, high, local_sem.at[1]),
        pltpu.make_async_copy(low_ref, low, local_sem.at[2]),
        pltpu.make_async_copy(high_z_ref, high_z, local_sem.at[3]),
        pltpu.make_async_copy(low_z_ref, low_z, local_sem.at[4]),
        pltpu.make_async_copy(outer_ref.at[sub], outer.at[pl.ds(sub * 64, 64)], local_sem.at[5]),
    ]
    for load in loads:
        load.start()

    def greet(sem, to_slab, to_sub):
        pl.semaphore_signal(sem, inc=1, device_id=(to_slab, to_sub), device_id_type=MESH)

    lines = slabs // LINE
    here, row = lax.rem(slab, LINE), lax.div(slab, LINE)
    column = [lax.rem(row + k, lines) * LINE + here for k in range(1, lines)]

    def greet_row(i, carry):
        target = row * LINE + lax.rem(here + i, LINE)
        for k in range(SUBS):
            greet(barrier, target, lax.rem(sub + k, SUBS))
        return carry

    for target in column:
        greet(barrier, target, sub)
    lax.fori_loop(1, LINE, greet_row, 0)
    for k in range(1, SUBS):
        greet(barrier, slab, lax.rem(sub + k, SUBS))
    loads[0].wait()
    density_rows(occupation_ref, sign_ref, orbitals, box)
    pl.semaphore_wait(barrier, LINE * SUBS - 1 + lines - 1)
    for target in column:
        greet(column_sem, target, sub)
    core_planes(span_ref, corner_ref, box, staged, core, meta, slab, sub)
    pl.semaphore_wait(column_sem, lines - 1)

    def pass_cores(j, carry):
        d = REACH - 1 - j
        to = lax.rem(slab + NEAR + d, slabs)
        send(meta.at[pl.ds(0, 1)], told.at[pl.ds(d, 1)], send_sem.at[1], recv_sem.at[1], to, sub)
        for q in range(SUBS):
            src = core.at[pl.ds((d * SUBS + q) * 8, 8)]
            dst = got.at[pl.ds((d * SUBS + sub) * 8, 8)]
            send(src, dst, send_sem.at[0], recv_sem.at[0], to, q)
        return carry

    def pass_outer(k, carry):
        to = lax.rem(sub + k, SUBS)
        dst = outer.at[pl.ds(sub * 64, 64)]
        send(outer_ref.at[to], dst, send_sem.at[2], recv_sem.at[2], slab, to)
        return carry

    lax.fori_loop(0, REACH, pass_cores, 0)
    lax.fori_loop(1, SUBS, pass_outer, 0)
    for load in loads[1:]:
        load.wait()
    wait_all(recv_sem.at[2], outer.at[pl.ds(0, 192)])
    for half in range(2):
        wide[half, pl.ds(0, NX), :] = outer[:, pl.ds(half * 128, 128)]
    wait_all(recv_sem.at[1], told)
    tell = pltpu.make_async_copy(told, first_cell, local_sem.at[6])
    tell.start()
    tell.wait()
    wait_all(recv_sem.at[0], got)
    place_cores(first_cell, got, ring, wide)

    density = jnp.concatenate([wide[half, pl.ds(0, NX), :] for half in range(2)], axis=1)
    table = (high[...], low[...])
    values = dot3(table, split(dot3(split(density), table)))
    spec[pl.ds(0, NX), :] = values[:, :128]
    spec[pl.ds(NX, NX), :] = values[:, 128:]

    to_everyone(spec, got_z, slab, sub, slabs, send_sem.at[3], recv_sem.at[3])
    outer[...] = exchange_correlation(density)
    me = slab * SUBS + sub
    shape = (count, 128)
    square = (
        wave_squares(rows(shape), count)
        + wave_squares(jnp.zeros(shape, jnp.int32) + lax.rem(me, NX), NX)
        + wave_squares(lanes(shape) + lax.div(me, NX) * 128, NY)
    )
    turned[...] = jnp.where(square > 0, 4.0 * math.pi / jnp.where(square > 0, square, 1.0), 0.0)
    wait_all(recv_sem.at[3], got_z.at[pl.ds(0, count - 1)])
    table_z = (high_z[...], low_z[...])
    values = dot3(table_z, split(got_z[...])) * turned[...]
    turned[...] = dot3(table_z, split(values))
    to_everyone(turned, back, slab, sub, slabs, send_sem.at[4], recv_sem.at[4])
    wait_all(recv_sem.at[4], back.at[pl.ds(0, count - 1)])

    values = jnp.concatenate([back[pl.ds(0, NX), :], back[pl.ds(NX, NX), :]], axis=1)
    values = dot3(split(dot3(table, split(values))), table) + outer[...]
    potential[...] = values
    for half in range(2):
        side = values[:, half * 128 : half * 128 + 128]
        wide[half, pl.ds(0, NX), :] = side
        wide[half, pl.ds(NX, BOX), :] = side[:BOX]

    def pass_plane(k, carry):
        to = lax.rem(sub + k, SUBS)
        src = potential.at[pl.ds(to * 64, 64)]
        send(src, grid_out.at[sub], send_sem.at[5], recv_sem.at[5], slab, to)
        return carry

    lax.fori_loop(1, SUBS, pass_plane, 0)

    column = lanes((24, 128))

    def windows_of(j, carry):
        swing = lax.div(j + 1, 2) * (1 - 2 * lax.rem(j, 2))
        d = jnp.where(j <= 8, 8 + swing, SPREAD - 1 - j)
        to = lax.rem(slab - d + slabs, slabs)
        for q in range(SUBS):
            fragment = to * SUBS + q
            start_x, start_y = corner_ref[1, fragment], corner_ref[2, fragment]
            here = pl.ds(start_x, BOX)
            strip = jnp.concatenate([wide[0, here, :], wide[1, here, :]], axis=1)
            strip = pltpu.roll(strip, (NY - start_y) % NY, 1)
            cut[pl.ds(q * BOX, BOX), :] = strip[:, :128]
        out = [jnp.zeros((24, 128), f32) for _ in range(3)]
        for b in range(8):
            tile, begin = b * BOX // 128, b * BOX % 128
            value = pltpu.roll(cut[pl.ds(b, 24, stride=8), :], begin, 1)
            here = (column >= begin) & (column < begin + BOX)
            out[tile] = jnp.where(here, value, out[tile])
            if begin + BOX > 128:
                out[tile + 1] = jnp.where(column < begin + BOX - 128, value, out[tile + 1])
        for t in range(3):
            windows[pl.ds(d * 72 + t, 24, stride=3), :] = out[t]

        for q in range(SUBS):
            src = windows.at[pl.ds((d * SUBS + q) * TILES, TILES)]
            dst = frame.at[pl.ds((d * SUBS + sub) * TILES, TILES)]

            @pl.when((d > 0) | (sub != q))
            def _():
                send(src, dst, send_sem.at[6], recv_sem.at[6], to, q)

        return carry

    lax.fori_loop(0, SPREAD, windows_of, 0)
    own = pl.ds(sub * TILES, TILES)
    keeps = [
        pltpu.make_async_copy(windows.at[own], frame.at[own], local_sem.at[0]),
        pltpu.make_async_copy(
            potential.at[pl.ds(sub * 64, 64)], grid_out.at[sub], local_sem.at[1]
        ),
    ]
    for keep in keeps:
        keep.start()
    own_windows = frame.at[pl.ds(0, (SPREAD * SUBS - 1) * TILES)]
    wait_all(recv_sem.at[6], own_windows)
    wait_all(recv_sem.at[5], grid_out.at[pl.ds(0, SUBS - 1)])
    wait_all(send_sem.at[0], got)
    wait_all(send_sem.at[1], told)
    wait_all(send_sem.at[2], outer.at[pl.ds(0, 192)])
    wait_all(send_sem.at[3], back.at[pl.ds(0, count - 1)])
    wait_all(send_sem.at[4], back.at[pl.ds(0, count - 1)])
    wait_all(send_sem.at[5], grid_out.at[pl.ds(0, SUBS - 1)])
    wait_all(send_sem.at[6], own_windows)
    for keep in keeps:
        keep.wait()


def finish_kernel(corner_ref, frame_ref, grid_ref, box_out, grid_out, box, grid, into, out):
    me = lax.axis_index("slab") * SUBS + lax.axis_index("sub")
    offset = corner_ref[0, me] % Z_DEV
    half = BOX * TILES // 2
    moves = [(frame_ref.at[pl.ds(offset * TILES + k * half, half)], box.at[pl.ds(k * half, half)]) for k in range(2)]
    moves.append((grid_ref, grid))
    ends = [box_out.at[pl.ds(0, half)], box_out.at[pl.ds(half, half)], grid_out]
    reads = [pltpu.make_async_copy(a, b, into.at[k]) for k, (a, b) in enumerate(moves)]
    writes = [pltpu.make_async_copy(moves[k][1], ends[k], out.at[k]) for k in range(3)]
    for read in reads:
        read.start()
    for read, write in zip(reads, writes):
        read.wait()
        write.start()
    for write in writes:
        write.wait()


def body(orbitals, occupations, patch_sign, corners, core_span, outer_density):
    count = lax.axis_size("slab") * SUBS
    tables = [jnp.asarray(t) for t in (*cas_table(NX), *cas_table(count))]
    smem = pl.BlockSpec(memory_space=pltpu.SMEM)
    hbm = pl.BlockSpec(memory_space=pl.ANY)
    cores = (REACH * SUBS * 8, 128)
    planes = (SPREAD * SUBS * TILES, 128)
    grid_shape = jax.ShapeDtypeStruct((Z_DEV, NX // SUBS, NY), f32)
    frame, potential = pl.pallas_call(
        whole_kernel,
        out_shape=[
            jax.ShapeDtypeStruct(planes, f32),
            grid_shape,
        ],
        in_specs=[smem] * 4 + [hbm] * 6,
        out_specs=[hbm] * 2,
        scratch_shapes=[
            pltpu.VMEM((BOX * TILES, 128), f32),
            pltpu.VMEM((384, 128), f32),
            pltpu.VMEM(cores, f32),
            pltpu.VMEM((8, 128), jnp.int32),
            pltpu.VMEM(cores, f32),
            pltpu.VMEM((REACH, 128), jnp.int32),
            pltpu.SMEM((REACH, 128), jnp.int32),
            pltpu.VMEM((NX, NY), f32),
            pltpu.VMEM((2, 2 * NX, 128), f32),
            pltpu.VMEM((2, NX + BOX, 128), f32),
            pltpu.VMEM((count, 128), f32),
            pltpu.VMEM((count, 128), f32),
            pltpu.VMEM((count, 128), f32),
            pltpu.VMEM((count, 128), f32),
            pltpu.VMEM((NX, NY), f32),
            pltpu.VMEM((SUBS * BOX, 128), f32),
            pltpu.VMEM(planes, f32),
            pltpu.SemaphoreType.DMA((7,)),
            pltpu.SemaphoreType.DMA((7,)),
            pltpu.SemaphoreType.DMA((7,)),
            pltpu.SemaphoreType.REGULAR,
            pltpu.VMEM((ORB, BOX * BOX * BOX), bf16),
            pltpu.VMEM((NX, NY), bf16),
            pltpu.VMEM((NX, NY), bf16),
            pltpu.VMEM((count, count), bf16),
            pltpu.VMEM((count, count), bf16),
        ],
        compiler_params=pltpu.CompilerParams(collective_id=0, has_side_effects=True),
        name="whole",
    )(core_span, corners.T, occupations, patch_sign.reshape(1, 1), orbitals[0], outer_density, *tables)
    box_potential, potential = pl.pallas_call(
        finish_kernel,
        out_shape=[jax.ShapeDtypeStruct((BOX * TILES, 128), f32), grid_shape],
        in_specs=[smem, hbm, hbm],
        out_specs=[hbm, hbm],
        scratch_shapes=[
            pltpu.VMEM((BOX * TILES, 128), f32),
            pltpu.VMEM(grid_shape.shape, f32),
            pltpu.SemaphoreType.DMA((3,)),
            pltpu.SemaphoreType.DMA((3,)),
        ],
        name="finish",
    )(corners.T, frame, potential)
    return box_potential.reshape(1, BOX * BOX * BOX), potential


def solution(mesh):
    placed = (
        P(("slab", "sub"), None, None),
        P(("slab", "sub"), None),
        P(("slab", "sub")),
        P(),
        P(("slab", "sub"), None),
        P("slab", "sub", None),
    )
    return jax.shard_map(
        body,
        mesh=mesh,
        in_specs=placed,
        out_specs=(P(("slab", "sub"), None), P("slab", "sub", None)),
        check_vma=False,
    )
```

```python
import math

import jax
import jax.numpy as jnp
import numpy as np
from jax import lax
from jax.experimental import pallas as pl
from jax.experimental.pallas import tpu as pltpu
from jax.sharding import PartitionSpec as P

BOX = 48
ORB = 16
NX = 256
NY = 256
Z_DEV = 4
SUBS = 4
LINE = 16
CORE = 32
FIRST = 8
SPACING = 0.35
FLOOR = 0.001
NEAR = FIRST // Z_DEV
REACH = 11
SPREAD = 13
TILES = BOX * BOX // 128
MESH = pl.DeviceIdType.MESH
f32 = jnp.float32
bf16 = jnp.bfloat16


def cas_table(count):
    index = np.arange(count)
    angle = 2.0 * np.pi * ((index[:, None] * index[None, :]) % count) / count
    table = (np.cos(angle) + np.sin(angle)) / np.sqrt(count)
    high = table.astype(np.float32).astype(bf16)
    low = (table - high.astype(np.float64)).astype(np.float32).astype(bf16)
    return high, low


def split(values):
    high = values.astype(bf16)
    return high, (values - high.astype(f32)).astype(bf16)


def dot(a, b):
    return jnp.dot(a, b, preferred_element_type=f32)


def dot3(a, b):
    return dot(a[0], b[0]) + (dot(a[0], b[1]) + dot(a[1], b[0]))


def lanes(shape):
    return lax.broadcasted_iota(jnp.int32, shape, len(shape) - 1)


def rows(shape):
    return lax.broadcasted_iota(jnp.int32, shape, 0)


def wait_all(sem, ref):
    pltpu.make_async_copy(ref, ref, sem).wait()


def send(src, dst, send_sem, recv_sem, slab, sub):
    pltpu.make_async_remote_copy(
        src, dst, send_sem, recv_sem, device_id=(slab, sub), device_id_type=MESH
    ).start()


def far_first(j, count):
    return count // 2 + lax.div(j + 1, 2) * (1 - 2 * lax.rem(j, 2))


def for_all_others(slab, sub, slabs, visit):
    subs = [sub] + [lax.rem(sub + k, SUBS) for k in range(1, SUBS)]
    lines, chips = slabs // LINE, LINE // 2
    row, chip, core = lax.div(slab, LINE), lax.div(lax.rem(slab, LINE), 2), lax.rem(slab, 2)

    for level in range(lines + chips - 2):

        def one(j, carry):
            to_row = lax.rem(row + far_first(j, lines), lines)
            to_chip = lax.rem(chip + far_first(level - j, chips), chips)
            base = (to_row * chips + to_chip) * 2
            for k in (2, 1, 3, 0):
                for c in range(2):
                    visit(base + c, subs[k])
            return carry

        lax.fori_loop(max(level - (chips - 1), 0), min(level, lines - 1) + 1, one, 0)
    for k in (2, 1, 3):
        visit(slab, subs[k])
    for k in (2, 1, 3, 0):
        visit(slab + 1 - 2 * core, subs[k])


def to_everyone(src, dst, slab, sub, slabs, send_sem, recv_sem):
    here = pl.ds(slab * SUBS + sub, 1)

    def visit(to_slab, to_sub):
        row = pl.ds(to_slab * SUBS + to_sub, 1)
        send(src.at[row], dst.at[here], send_sem, recv_sem, to_slab, to_sub)

    for_all_others(slab, sub, slabs, visit)
    dst[here, :] = src[here, :]


def wave_squares(index, count):
    folded = jnp.where(index > count // 2, index - count, index)
    wave = (2.0 * math.pi / (count * SPACING)) * folded.astype(f32)
    return wave * wave


def exchange_correlation(density):
    clipped = jnp.maximum(density, FLOOR)
    root = jnp.exp(jnp.log(clipped) * (1.0 / 3.0))
    radius = (3.0 / (4.0 * math.pi)) ** (1.0 / 3.0) / root
    exchange = -((3.0 / math.pi) ** (1.0 / 3.0)) * root
    inverse = 1.0 / (radius + 7.8)
    return exchange - 0.44 * inverse - (0.44 / 3.0) * radius * inverse * inverse


def density_rows(occupation_ref, sign_ref, orbital_ref, box):
    row = rows((ORB, 128))
    weight = jnp.zeros((ORB, 128), jnp.int32)
    for o in range(ORB):
        weight = jnp.where(row == o, occupation_ref[0, o] * sign_ref[0, 0], weight)
    weight = weight.astype(f32)

    def one(g, carry):
        base = pl.multiple_of(g * 1024, 1024)
        values = orbital_ref[:, pl.ds(base, 1024)].astype(f32)
        out = pl.multiple_of(g * 8, 8)
        for j in range(8):
            part = values[:, j * 128 : j * 128 + 128]
            box[pl.ds(out + j, 1), :] = jnp.sum(weight * (part * part), axis=0, keepdims=True)
        return carry

    lax.fori_loop(FIRST * TILES // 8, BOX * TILES // 8, one, 0, unroll=2)


def core_planes(span_ref, corner_ref, box, staged, core, meta, slab, sub):
    own = slab * SUBS + sub
    first_z, first_x, first_y = span_ref[0, 0], span_ref[0, 1], span_ref[0, 2]
    long_z, long_x, long_y = span_ref[0, 3], span_ref[0, 4], span_ref[0, 5]
    offset = corner_ref[0, own] % Z_DEV
    planes = BOX - FIRST
    start = first_x * BOX + first_y
    tile, lane = start // 128, start % 128
    shape = (planes, 128)
    column = lanes(shape)
    turned = []
    for t in range(13):
        row = FIRST * TILES + jnp.minimum(tile + t, TILES - 1)
        raw = box[pl.ds(row, planes, stride=TILES), :]
        turned.append(pltpu.roll(raw, (128 - lane) % 128, 1))
    chunks = [jnp.where(column < 128 - lane, turned[t], turned[t + 1]) for t in range(12)]
    plane = rows(shape) + FIRST
    within_z = (plane >= first_z) & (plane < first_z + long_z)
    staged[pl.ds(0, 32), :] = jnp.zeros((32, 128), f32)
    staged[pl.ds(352, 32), :] = jnp.zeros((32, 128), f32)
    for t in range(8):
        value = jnp.zeros(shape, f32)
        for m in range(4):
            source = (4 * t + m) * BOX
            chunk, begin = source // 128, source % 128
            shift = (32 * m - begin) % 128
            piece = pltpu.roll(chunks[chunk], shift, 1)
            if begin + CORE > 128:
                after = pltpu.roll(chunks[chunk + 1], shift, 1)
                piece = jnp.where(column < 32 * m + 128 - begin, piece, after)
            value = jnp.where(column // 32 == m, piece, value)
        inside = within_z & (4 * t + column // 32 < long_x) & (column % 32 < long_y)
        staged[pl.ds(32 + t, planes, stride=8), :] = jnp.where(inside, value, 0.0)
    core[...] = staged[pl.ds((Z_DEV - offset) * 8, REACH * SUBS * 8), :]
    start_x = (corner_ref[1, own] + first_x) % NX
    start_y = (corner_ref[2, own] + first_y) % NY
    meta[...] = jnp.where(lanes((8, 128)) == 0, start_x, start_y)


def place_cores(first_cell, got, ring, wide, spans):
    column = lanes((8, 128))

    def place(d, carry):
        base = pl.multiple_of(d * 32, 32)
        cells = got[pl.ds(base, 8), :]
        for q in range(1, SUBS):
            cells = cells + got[pl.ds(base + 8 * q, 8), :]
        start_x, start_y = first_cell[d, 0], first_cell[d, 1]
        for m in range(4):
            piece = pltpu.roll(cells, (128 - 32 * m) % 128, 1)
            piece = jnp.where(column < 32, piece, 0.0)
            piece = jnp.concatenate([piece, jnp.zeros((8, 128), f32)], axis=1)
            piece = pltpu.roll(piece, start_y, 1)
            for half in range(2):
                side = piece[:, half * 128 : half * 128 + 128]
                ring[half, pl.ds(m, 8, stride=4), :] = side
                ring[half, pl.ds(NX + m, 8, stride=4), :] = side
        for half in range(2):
            wide[half, pl.ds(0, NX), :] = (
                wide[half, pl.ds(0, NX), :] + ring[half, pl.ds(NX - start_x, NX), :]
            )
        return carry

    for span in spans:
        lax.fori_loop(*span, place, 0)


def whole_kernel(
    span_ref,
    corner_ref,
    occupation_ref,
    sign_ref,
    orbital_ref,
    outer_ref,
    high_ref,
    low_ref,
    high_z_ref,
    low_z_ref,
    frame,
    grid_out,
    box,
    staged,
    core,
    meta,
    got,
    told,
    first_cell,
    outer,
    ring,
    wide,
    spec,
    got_z,
    turned,
    back,
    potential,
    cut,
    windows,
    send_sem,
    recv_sem,
    local_sem,
    column_sem,
    orbitals,
    high,
    low,
    high_z,
    low_z,
):
    slab, sub = lax.axis_index("slab"), lax.axis_index("sub")
    slabs = lax.axis_size("slab")
    count = slabs * SUBS
    barrier = pltpu.get_barrier_semaphore()

    loads = [
        pltpu.make_async_copy(orbital_ref, orbitals, local_sem.at[0]),
        pltpu.make_async_copy(high_ref, high, local_sem.at[1]),
        pltpu.make_async_copy(low_ref, low, local_sem.at[2]),
        pltpu.make_async_copy(high_z_ref, high_z, local_sem.at[3]),
        pltpu.make_async_copy(low_z_ref, low_z, local_sem.at[4]),
        pltpu.make_async_copy(outer_ref.at[sub], outer.at[pl.ds(sub * 64, 64)], local_sem.at[5]),
    ]
    for load in loads:
        load.start()

    def greet(sem, to_slab, to_sub):
        pl.semaphore_signal(sem, inc=1, device_id=(to_slab, to_sub), device_id_type=MESH)

    lines = slabs // LINE
    here, row = lax.rem(slab, LINE), lax.div(slab, LINE)
    column = [lax.rem(row + k, lines) * LINE + here for k in range(1, lines)]

    def greet_row(i, carry):
        target = row * LINE + lax.rem(here + i, LINE)
        for k in range(SUBS):
            greet(barrier, target, lax.rem(sub + k, SUBS))
        return carry

    for target in column:
        greet(barrier, target, sub)
    lax.fori_loop(1, LINE, greet_row, 0)
    for k in range(1, SUBS):
        greet(barrier, slab, lax.rem(sub + k, SUBS))
    loads[0].wait()
    density_rows(occupation_ref, sign_ref, orbitals, box)
    pl.semaphore_wait(barrier, LINE * SUBS - 1 + lines - 1)
    for target in column:
        greet(column_sem, target, sub)
    core_planes(span_ref, corner_ref, box, staged, core, meta, slab, sub)
    pl.semaphore_wait(column_sem, lines - 1)

    batches = (((4, 9),), ((0, 4), (9, REACH)))

    def pass_cores(batch):
        def one(d, carry):
            to = lax.rem(slab + NEAR + d, slabs)
            recv = recv_sem.at[7 + 2 * batch]
            send(meta.at[pl.ds(0, 1)], told.at[pl.ds(d, 1)], send_sem.at[1], recv, to, sub)
            for q in range(SUBS):
                src = core.at[pl.ds((d * SUBS + q) * 8, 8)]
                dst = got.at[pl.ds((d * SUBS + sub) * 8, 8)]
                send(src, dst, send_sem.at[0], recv_sem.at[8 + 2 * batch], to, q)
            return carry

        for span in batches[batch]:
            lax.fori_loop(*span, one, 0)

    def pass_outer(k, carry):
        to = lax.rem(sub + k, SUBS)
        dst = outer.at[pl.ds(sub * 64, 64)]
        send(outer_ref.at[to], dst, send_sem.at[2], recv_sem.at[2], slab, to)
        return carry

    pass_cores(0)
    pass_cores(1)
    lax.fori_loop(1, SUBS, pass_outer, 0)
    ring[...] = jnp.zeros_like(ring)
    for load in loads[1:]:
        load.wait()
    wait_all(recv_sem.at[2], outer.at[pl.ds(0, 192)])
    for half in range(2):
        wide[half, pl.ds(0, NX), :] = outer[:, pl.ds(half * 128, 128)]
    for batch in (1, 0):
        spans = batches[batch]
        size = sum(end - start for start, end in spans)
        wait_all(recv_sem.at[7 + 2 * batch], told.at[pl.ds(0, size)])
        tells = []
        for k, (start, end) in enumerate(spans):
            part = pl.ds(start, end - start)
            sem = local_sem.at[6 + batch + k]
            tells.append(pltpu.make_async_copy(told.at[part], first_cell.at[part], sem))
            tells[-1].start()
        for tell in tells:
            tell.wait()
        wait_all(recv_sem.at[8 + 2 * batch], got.at[pl.ds(0, size * SUBS * 8)])
        place_cores(first_cell, got, ring, wide, spans)

    density = jnp.concatenate([wide[half, pl.ds(0, NX), :] for half in range(2)], axis=1)
    table = (high[...], low[...])
    values = dot3(table, split(dot3(split(density), table)))
    spec[pl.ds(0, NX), :] = values[:, :128]
    spec[pl.ds(NX, NX), :] = values[:, 128:]

    to_everyone(spec, got_z, slab, sub, slabs, send_sem.at[3], recv_sem.at[3])
    outer[...] = exchange_correlation(density)
    me = slab * SUBS + sub
    shape = (count, 128)
    square = (
        wave_squares(rows(shape), count)
        + wave_squares(jnp.zeros(shape, jnp.int32) + lax.rem(me, NX), NX)
        + wave_squares(lanes(shape) + lax.div(me, NX) * 128, NY)
    )
    turned[...] = jnp.where(square > 0, 4.0 * math.pi / jnp.where(square > 0, square, 1.0), 0.0)
    wait_all(recv_sem.at[3], got_z.at[pl.ds(0, count - 1)])
    table_z = (high_z[...], low_z[...])
    values = dot3(table_z, split(got_z[...])) * turned[...]
    turned[...] = dot3(table_z, split(values))
    to_everyone(turned, back, slab, sub, slabs, send_sem.at[4], recv_sem.at[4])
    wait_all(recv_sem.at[4], back.at[pl.ds(0, count - 1)])

    values = jnp.concatenate([back[pl.ds(0, NX), :], back[pl.ds(NX, NX), :]], axis=1)
    values = dot3(split(dot3(table, split(values))), table) + outer[...]
    potential[...] = values
    for half in range(2):
        side = values[:, half * 128 : half * 128 + 128]
        wide[half, pl.ds(0, NX), :] = side
        wide[half, pl.ds(NX, BOX), :] = side[:BOX]

    def pass_plane(k, carry):
        to = lax.rem(sub + k, SUBS)
        src = potential.at[pl.ds(to * 64, 64)]
        send(src, grid_out.at[sub], send_sem.at[5], recv_sem.at[5], slab, to)
        return carry

    lax.fori_loop(1, SUBS, pass_plane, 0)

    column = lanes((24, 128))

    def windows_of(j, carry):
        swing = lax.div(j + 1, 2) * (1 - 2 * lax.rem(j, 2))
        d = jnp.where(j <= 8, 8 + swing, SPREAD - 1 - j)
        to = lax.rem(slab - d + slabs, slabs)
        for q in range(SUBS):
            fragment = to * SUBS + q
            start_x, start_y = corner_ref[1, fragment], corner_ref[2, fragment]
            here = pl.ds(start_x, BOX)
            strip = jnp.concatenate([wide[0, here, :], wide[1, here, :]], axis=1)
            strip = pltpu.roll(strip, (NY - start_y) % NY, 1)
            cut[pl.ds(q * BOX, BOX), :] = strip[:, :128]
        out = [jnp.zeros((24, 128), f32) for _ in range(3)]
        for b in range(8):
            tile, begin = b * BOX // 128, b * BOX % 128
            value = pltpu.roll(cut[pl.ds(b, 24, stride=8), :], begin, 1)
            here = (column >= begin) & (column < begin + BOX)
            out[tile] = jnp.where(here, value, out[tile])
            if begin + BOX > 128:
                out[tile + 1] = jnp.where(column < begin + BOX - 128, value, out[tile + 1])
        for t in range(3):
            windows[pl.ds(d * 72 + t, 24, stride=3), :] = out[t]

        for q in range(SUBS):
            src = windows.at[pl.ds((d * SUBS + q) * TILES, TILES)]
            dst = frame.at[pl.ds((d * SUBS + sub) * TILES, TILES)]

            @pl.when((d > 0) | (sub != q))
            def _():
                send(src, dst, send_sem.at[6], recv_sem.at[6], to, q)

        return carry

    lax.fori_loop(0, SPREAD, windows_of, 0)
    own = pl.ds(sub * TILES, TILES)
    keeps = [
        pltpu.make_async_copy(windows.at[own], frame.at[own], local_sem.at[0]),
        pltpu.make_async_copy(
            potential.at[pl.ds(sub * 64, 64)], grid_out.at[sub], local_sem.at[1]
        ),
    ]
    for keep in keeps:
        keep.start()
    own_windows = frame.at[pl.ds(0, (SPREAD * SUBS - 1) * TILES)]
    wait_all(recv_sem.at[6], own_windows)
    wait_all(recv_sem.at[5], grid_out.at[pl.ds(0, SUBS - 1)])
    wait_all(send_sem.at[0], got)
    wait_all(send_sem.at[1], told)
    wait_all(send_sem.at[2], outer.at[pl.ds(0, 192)])
    wait_all(send_sem.at[3], back.at[pl.ds(0, count - 1)])
    wait_all(send_sem.at[4], back.at[pl.ds(0, count - 1)])
    wait_all(send_sem.at[5], grid_out.at[pl.ds(0, SUBS - 1)])
    wait_all(send_sem.at[6], own_windows)
    for keep in keeps:
        keep.wait()


def finish_kernel(corner_ref, frame_ref, grid_ref, box_out, grid_out, box, grid, into, out):
    me = lax.axis_index("slab") * SUBS + lax.axis_index("sub")
    offset = corner_ref[0, me] % Z_DEV
    half = BOX * TILES // 2
    moves = [(frame_ref.at[pl.ds(offset * TILES + k * half, half)], box.at[pl.ds(k * half, half)]) for k in range(2)]
    moves.append((grid_ref, grid))
    ends = [box_out.at[pl.ds(0, half)], box_out.at[pl.ds(half, half)], grid_out]
    reads = [pltpu.make_async_copy(a, b, into.at[k]) for k, (a, b) in enumerate(moves)]
    writes = [pltpu.make_async_copy(moves[k][1], ends[k], out.at[k]) for k in range(3)]
    for read in reads:
        read.start()
    for read, write in zip(reads, writes):
        read.wait()
        write.start()
    for write in writes:
        write.wait()


def body(orbitals, occupations, patch_sign, corners, core_span, outer_density):
    count = lax.axis_size("slab") * SUBS
    tables = [jnp.asarray(t) for t in (*cas_table(NX), *cas_table(count))]
    smem = pl.BlockSpec(memory_space=pltpu.SMEM)
    hbm = pl.BlockSpec(memory_space=pl.ANY)
    cores = (REACH * SUBS * 8, 128)
    planes = (SPREAD * SUBS * TILES, 128)
    grid_shape = jax.ShapeDtypeStruct((Z_DEV, NX // SUBS, NY), f32)
    frame, potential = pl.pallas_call(
        whole_kernel,
        out_shape=[
            jax.ShapeDtypeStruct(planes, f32),
            grid_shape,
        ],
        in_specs=[smem] * 4 + [hbm] * 6,
        out_specs=[hbm] * 2,
        scratch_shapes=[
            pltpu.VMEM((BOX * TILES, 128), f32),
            pltpu.VMEM((384, 128), f32),
            pltpu.VMEM(cores, f32),
            pltpu.VMEM((8, 128), jnp.int32),
            pltpu.VMEM(cores, f32),
            pltpu.VMEM((REACH, 128), jnp.int32),
            pltpu.SMEM((REACH, 128), jnp.int32),
            pltpu.VMEM((NX, NY), f32),
            pltpu.VMEM((2, 2 * NX, 128), f32),
            pltpu.VMEM((2, NX + BOX, 128), f32),
            pltpu.VMEM((count, 128), f32),
            pltpu.VMEM((count, 128), f32),
            pltpu.VMEM((count, 128), f32),
            pltpu.VMEM((count, 128), f32),
            pltpu.VMEM((NX, NY), f32),
            pltpu.VMEM((SUBS * BOX, 128), f32),
            pltpu.VMEM(planes, f32),
            pltpu.SemaphoreType.DMA((7,)),
            pltpu.SemaphoreType.DMA((11,)),
            pltpu.SemaphoreType.DMA((9,)),
            pltpu.SemaphoreType.REGULAR,
            pltpu.VMEM((ORB, BOX * BOX * BOX), bf16),
            pltpu.VMEM((NX, NY), bf16),
            pltpu.VMEM((NX, NY), bf16),
            pltpu.VMEM((count, count), bf16),
            pltpu.VMEM((count, count), bf16),
        ],
        compiler_params=pltpu.CompilerParams(collective_id=0, has_side_effects=True),
        name="whole",
    )(core_span, corners.T, occupations, patch_sign.reshape(1, 1), orbitals[0], outer_density, *tables)
    box_potential, potential = pl.pallas_call(
        finish_kernel,
        out_shape=[jax.ShapeDtypeStruct((BOX * TILES, 128), f32), grid_shape],
        in_specs=[smem, hbm, hbm],
        out_specs=[hbm, hbm],
        scratch_shapes=[
            pltpu.VMEM((BOX * TILES, 128), f32),
            pltpu.VMEM(grid_shape.shape, f32),
            pltpu.SemaphoreType.DMA((3,)),
            pltpu.SemaphoreType.DMA((3,)),
        ],
        name="finish",
    )(corners.T, frame, potential)
    return box_potential.reshape(1, BOX * BOX * BOX), potential


def solution(mesh):
    placed = (
        P(("slab", "sub"), None, None),
        P(("slab", "sub"), None),
        P(("slab", "sub")),
        P(),
        P(("slab", "sub"), None),
        P("slab", "sub", None),
    )
    return jax.shard_map(
        body,
        mesh=mesh,
        in_specs=placed,
        out_specs=(P(("slab", "sub"), None), P("slab", "sub", None)),
        check_vma=False,
    )
```

```python
import math

import jax
import jax.numpy as jnp
import numpy as np
from jax import lax
from jax.experimental import pallas as pl
from jax.experimental.pallas import tpu as pltpu
from jax.sharding import PartitionSpec as P

BOX = 48
ORB = 16
NX = 256
NY = 256
Z_DEV = 4
SUBS = 4
LINE = 16
CORE = 32
FIRST = 8
SPACING = 0.35
FLOOR = 0.001
NEAR = FIRST // Z_DEV
REACH = 11
SPREAD = 13
TILES = BOX * BOX // 128
MESH = pl.DeviceIdType.MESH
f32 = jnp.float32
bf16 = jnp.bfloat16


def cas_table(count):
    index = np.arange(count)
    angle = 2.0 * np.pi * ((index[:, None] * index[None, :]) % count) / count
    table = (np.cos(angle) + np.sin(angle)) / np.sqrt(count)
    high = table.astype(np.float32).astype(bf16)
    low = (table - high.astype(np.float64)).astype(np.float32).astype(bf16)
    return high, low


def split(values):
    high = values.astype(bf16)
    return high, (values - high.astype(f32)).astype(bf16)


def dot(a, b):
    return jnp.dot(a, b, preferred_element_type=f32)


def dot3(a, b):
    return dot(a[0], b[0]) + (dot(a[0], b[1]) + dot(a[1], b[0]))


def lanes(shape):
    return lax.broadcasted_iota(jnp.int32, shape, len(shape) - 1)


def rows(shape):
    return lax.broadcasted_iota(jnp.int32, shape, 0)


def wait_all(sem, ref):
    pltpu.make_async_copy(ref, ref, sem).wait()


def send(src, dst, send_sem, recv_sem, slab, sub):
    pltpu.make_async_remote_copy(
        src, dst, send_sem, recv_sem, device_id=(slab, sub), device_id_type=MESH
    ).start()


def far_first(j, count):
    return count // 2 + lax.div(j + 1, 2) * (1 - 2 * lax.rem(j, 2))


def for_all_others(slab, sub, slabs, visit):
    subs = [sub] + [lax.rem(sub + k, SUBS) for k in range(1, SUBS)]
    lines, chips = slabs // LINE, LINE // 2
    row, chip, core = lax.div(slab, LINE), lax.div(lax.rem(slab, LINE), 2), lax.rem(slab, 2)

    for level in range(lines + chips - 2):

        def one(j, carry):
            to_row = lax.rem(row + far_first(j, lines), lines)
            to_chip = lax.rem(chip + far_first(level - j, chips), chips)
            base = (to_row * chips + to_chip) * 2
            for k in (2, 1, 3, 0):
                for c in range(2):
                    visit(base + c, subs[k])
            return carry

        lax.fori_loop(max(level - (chips - 1), 0), min(level, lines - 1) + 1, one, 0)
    for k in (2, 1, 3):
        visit(slab, subs[k])
    for k in (2, 1, 3, 0):
        visit(slab + 1 - 2 * core, subs[k])


def to_everyone(src, dst, slab, sub, slabs, send_sem, recv_sem):
    here = pl.ds(slab * SUBS + sub, 1)

    def visit(to_slab, to_sub):
        row = pl.ds(to_slab * SUBS + to_sub, 1)
        send(src.at[row], dst.at[here], send_sem, recv_sem, to_slab, to_sub)

    for_all_others(slab, sub, slabs, visit)
    dst[here, :] = src[here, :]


def wave_squares(index, count):
    folded = jnp.where(index > count // 2, index - count, index)
    wave = (2.0 * math.pi / (count * SPACING)) * folded.astype(f32)
    return wave * wave


def exchange_correlation(density):
    clipped = jnp.maximum(density, FLOOR)
    root = jnp.exp(jnp.log(clipped) * (1.0 / 3.0))
    radius = (3.0 / (4.0 * math.pi)) ** (1.0 / 3.0) / root
    exchange = -((3.0 / math.pi) ** (1.0 / 3.0)) * root
    inverse = 1.0 / (radius + 7.8)
    return exchange - 0.44 * inverse - (0.44 / 3.0) * radius * inverse * inverse


def density_rows(occupation_ref, sign_ref, orbital_ref, box):
    row = rows((ORB, 128))
    weight = jnp.zeros((ORB, 128), jnp.int32)
    for o in range(ORB):
        weight = jnp.where(row == o, occupation_ref[0, o] * sign_ref[0, 0], weight)
    weight = weight.astype(f32)

    def one(g, carry):
        base = pl.multiple_of(g * 1024, 1024)
        values = orbital_ref[:, pl.ds(base, 1024)].astype(f32)
        out = pl.multiple_of(g * 8, 8)
        for j in range(8):
            part = values[:, j * 128 : j * 128 + 128]
            box[pl.ds(out + j, 1), :] = jnp.sum(weight * (part * part), axis=0, keepdims=True)
        return carry

    lax.fori_loop(FIRST * TILES // 8, BOX * TILES // 8, one, 0, unroll=2)


def core_planes(span_ref, corner_ref, box, staged, core, meta, slab, sub):
    own = slab * SUBS + sub
    first_z, first_x, first_y = span_ref[0, 0], span_ref[0, 1], span_ref[0, 2]
    long_z, long_x, long_y = span_ref[0, 3], span_ref[0, 4], span_ref[0, 5]
    offset = corner_ref[0, own] % Z_DEV
    planes = BOX - FIRST
    start = first_x * BOX + first_y
    tile, lane = start // 128, start % 128
    shape = (planes, 128)
    column = lanes(shape)
    turned = []
    for t in range(13):
        row = FIRST * TILES + jnp.minimum(tile + t, TILES - 1)
        raw = box[pl.ds(row, planes, stride=TILES), :]
        turned.append(pltpu.roll(raw, (128 - lane) % 128, 1))
    chunks = [jnp.where(column < 128 - lane, turned[t], turned[t + 1]) for t in range(12)]
    plane = rows(shape) + FIRST
    within_z = (plane >= first_z) & (plane < first_z + long_z)
    staged[pl.ds(0, 32), :] = jnp.zeros((32, 128), f32)
    staged[pl.ds(352, 32), :] = jnp.zeros((32, 128), f32)
    for t in range(8):
        value = jnp.zeros(shape, f32)
        for m in range(4):
            source = (4 * t + m) * BOX
            chunk, begin = source // 128, source % 128
            shift = (32 * m - begin) % 128
            piece = pltpu.roll(chunks[chunk], shift, 1)
            if begin + CORE > 128:
                after = pltpu.roll(chunks[chunk + 1], shift, 1)
                piece = jnp.where(column < 32 * m + 128 - begin, piece, after)
            value = jnp.where(column // 32 == m, piece, value)
        inside = within_z & (4 * t + column // 32 < long_x) & (column % 32 < long_y)
        staged[pl.ds(32 + t, planes, stride=8), :] = jnp.where(inside, value, 0.0)
    core[...] = staged[pl.ds((Z_DEV - offset) * 8, REACH * SUBS * 8), :]
    start_x = (corner_ref[1, own] + first_x) % NX
    start_y = (corner_ref[2, own] + first_y) % NY
    meta[...] = jnp.where(lanes((8, 128)) == 0, start_x, start_y)


def place_cores(first_cell, got, ring, wide, spans):
    column = lanes((8, 128))

    def place(d, carry):
        base = pl.multiple_of(d * 32, 32)
        cells = got[pl.ds(base, 8), :]
        for q in range(1, SUBS):
            cells = cells + got[pl.ds(base + 8 * q, 8), :]
        start_x, start_y = first_cell[d, 0], first_cell[d, 1]
        for m in range(4):
            piece = pltpu.roll(cells, (128 - 32 * m) % 128, 1)
            piece = jnp.where(column < 32, piece, 0.0)
            piece = jnp.concatenate([piece, jnp.zeros((8, 128), f32)], axis=1)
            piece = pltpu.roll(piece, start_y, 1)
            for half in range(2):
                side = piece[:, half * 128 : half * 128 + 128]
                ring[half, pl.ds(m, 8, stride=4), :] = side
                ring[half, pl.ds(NX + m, 8, stride=4), :] = side
        for half in range(2):
            wide[half, pl.ds(0, NX), :] = (
                wide[half, pl.ds(0, NX), :] + ring[half, pl.ds(NX - start_x, NX), :]
            )
        return carry

    for span in spans:
        lax.fori_loop(*span, place, 0)


def whole_kernel(
    span_ref,
    corner_ref,
    occupation_ref,
    sign_ref,
    orbital_ref,
    outer_ref,
    high_ref,
    low_ref,
    high_z_ref,
    low_z_ref,
    frame,
    grid_out,
    box,
    staged,
    core,
    meta,
    got,
    told,
    first_cell,
    outer,
    ring,
    wide,
    spec,
    got_z,
    turned,
    back,
    potential,
    cut,
    windows,
    send_sem,
    recv_sem,
    local_sem,
    column_sem,
    orbitals,
    high,
    low,
    high_z,
    low_z,
):
    slab, sub = lax.axis_index("slab"), lax.axis_index("sub")
    slabs = lax.axis_size("slab")
    count = slabs * SUBS
    barrier = pltpu.get_barrier_semaphore()

    loads = [
        pltpu.make_async_copy(orbital_ref, orbitals, local_sem.at[0]),
        pltpu.make_async_copy(high_ref, high, local_sem.at[1]),
        pltpu.make_async_copy(low_ref, low, local_sem.at[2]),
        pltpu.make_async_copy(high_z_ref, high_z, local_sem.at[3]),
        pltpu.make_async_copy(low_z_ref, low_z, local_sem.at[4]),
        pltpu.make_async_copy(outer_ref.at[sub], outer.at[pl.ds(sub * 64, 64)], local_sem.at[5]),
    ]
    for load in loads:
        load.start()

    def greet(sem, to_slab, to_sub):
        pl.semaphore_signal(sem, inc=1, device_id=(to_slab, to_sub), device_id_type=MESH)

    lines = slabs // LINE
    here, row = lax.rem(slab, LINE), lax.div(slab, LINE)
    column = [lax.rem(row + k, lines) * LINE + here for k in range(1, lines)]

    def greet_row(i, carry):
        target = row * LINE + lax.rem(here + i, LINE)
        for k in range(SUBS):
            greet(barrier, target, lax.rem(sub + k, SUBS))
        return carry

    for target in column:
        greet(barrier, target, sub)
    lax.fori_loop(1, LINE, greet_row, 0)
    for k in range(1, SUBS):
        greet(barrier, slab, lax.rem(sub + k, SUBS))
    loads[0].wait()
    density_rows(occupation_ref, sign_ref, orbitals, box)
    pl.semaphore_wait(barrier, LINE * SUBS - 1 + lines - 1)
    for target in column:
        greet(column_sem, target, sub)
    core_planes(span_ref, corner_ref, box, staged, core, meta, slab, sub)
    pl.semaphore_wait(column_sem, lines - 1)

    batches = (((4, 9),), ((0, 4), (9, REACH)))

    def pass_cores(batch):
        def one(d, carry):
            to = lax.rem(slab + NEAR + d, slabs)
            recv = recv_sem.at[7 + 2 * batch]
            send(meta.at[pl.ds(0, 1)], told.at[pl.ds(d, 1)], send_sem.at[1], recv, to, sub)
            for q in range(SUBS):
                src = core.at[pl.ds((d * SUBS + q) * 8, 8)]
                dst = got.at[pl.ds((d * SUBS + sub) * 8, 8)]
                send(src, dst, send_sem.at[0], recv_sem.at[8 + 2 * batch], to, q)
            return carry

        for span in batches[batch]:
            lax.fori_loop(*span, one, 0)

    def pass_outer(k, carry):
        to = lax.rem(sub + k, SUBS)
        dst = outer.at[pl.ds(sub * 64, 64)]
        send(outer_ref.at[to], dst, send_sem.at[2], recv_sem.at[2], slab, to)
        return carry

    pass_cores(0)
    pass_cores(1)
    lax.fori_loop(1, SUBS, pass_outer, 0)
    ring[...] = jnp.zeros_like(ring)
    for load in loads[1:]:
        load.wait()
    wait_all(recv_sem.at[2], outer.at[pl.ds(0, 192)])
    for half in range(2):
        wide[half, pl.ds(0, NX), :] = outer[:, pl.ds(half * 128, 128)]
    for batch in (1, 0):
        spans = batches[batch]
        size = sum(end - start for start, end in spans)
        wait_all(recv_sem.at[7 + 2 * batch], told.at[pl.ds(0, size)])
        tells = []
        for k, (start, end) in enumerate(spans):
            part = pl.ds(start, end - start)
            sem = local_sem.at[6 + batch + k]
            tells.append(pltpu.make_async_copy(told.at[part], first_cell.at[part], sem))
            tells[-1].start()
        for tell in tells:
            tell.wait()
        wait_all(recv_sem.at[8 + 2 * batch], got.at[pl.ds(0, size * SUBS * 8)])
        place_cores(first_cell, got, ring, wide, spans)

    density = jnp.concatenate([wide[half, pl.ds(0, NX), :] for half in range(2)], axis=1)
    table = (high[...], low[...])
    values = dot3(table, split(dot3(split(density), table)))
    spec[pl.ds(0, NX), :] = values[:, :128]
    spec[pl.ds(NX, NX), :] = values[:, 128:]

    to_everyone(spec, got_z, slab, sub, slabs, send_sem.at[3], recv_sem.at[3])
    outer[...] = exchange_correlation(density)
    me = slab * SUBS + sub
    shape = (count, 128)
    square = (
        wave_squares(rows(shape), count)
        + wave_squares(jnp.zeros(shape, jnp.int32) + lax.rem(me, NX), NX)
        + wave_squares(lanes(shape) + lax.div(me, NX) * 128, NY)
    )
    turned[...] = jnp.where(square > 0, 4.0 * math.pi / jnp.where(square > 0, square, 1.0), 0.0)
    wait_all(recv_sem.at[3], got_z.at[pl.ds(0, count - 1)])
    table_z = (high_z[...], low_z[...])
    values = dot3(table_z, split(got_z[...])) * turned[...]
    turned[...] = dot3(table_z, split(values))
    to_everyone(turned, back, slab, sub, slabs, send_sem.at[4], recv_sem.at[4])
    wait_all(recv_sem.at[4], back.at[pl.ds(0, count - 1)])

    values = jnp.concatenate([back[pl.ds(0, NX), :], back[pl.ds(NX, NX), :]], axis=1)
    values = dot3(split(dot3(table, split(values))), table) + outer[...]
    potential[...] = values
    for half in range(2):
        side = values[:, half * 128 : half * 128 + 128]
        wide[half, pl.ds(0, NX), :] = side
        wide[half, pl.ds(NX, BOX), :] = side[:BOX]

    def pass_plane(k, carry):
        to = lax.rem(sub + k, SUBS)
        src = potential.at[pl.ds(to * 64, 64)]
        send(src, grid_out.at[sub], send_sem.at[5], recv_sem.at[5], slab, to)
        return carry

    lax.fori_loop(1, SUBS, pass_plane, 0)

    column = lanes((24, 128))

    def windows_of(j, carry):
        d = SPREAD - 1 - j
        to = lax.rem(slab - d + slabs, slabs)
        for q in range(SUBS):
            fragment = to * SUBS + q
            start_x, start_y = corner_ref[1, fragment], corner_ref[2, fragment]
            here = pl.ds(start_x, BOX)
            strip = jnp.concatenate([wide[0, here, :], wide[1, here, :]], axis=1)
            strip = pltpu.roll(strip, (NY - start_y) % NY, 1)
            cut[pl.ds(q * BOX, BOX), :] = strip[:, :128]
        out = [jnp.zeros((24, 128), f32) for _ in range(3)]
        for b in range(8):
            tile, begin = b * BOX // 128, b * BOX % 128
            value = pltpu.roll(cut[pl.ds(b, 24, stride=8), :], begin, 1)
            here = (column >= begin) & (column < begin + BOX)
            out[tile] = jnp.where(here, value, out[tile])
            if begin + BOX > 128:
                out[tile + 1] = jnp.where(column < begin + BOX - 128, value, out[tile + 1])
        for t in range(3):
            windows[pl.ds(d * 72 + t, 24, stride=3), :] = out[t]

        for q in range(SUBS):
            src = windows.at[pl.ds((d * SUBS + q) * TILES, TILES)]
            dst = frame.at[pl.ds((d * SUBS + sub) * TILES, TILES)]

            @pl.when((d > 0) | (sub != q))
            def _():
                send(src, dst, send_sem.at[6], recv_sem.at[6], to, q)

        return carry

    lax.fori_loop(0, SPREAD, windows_of, 0)
    own = pl.ds(sub * TILES, TILES)
    keeps = [
        pltpu.make_async_copy(windows.at[own], frame.at[own], local_sem.at[0]),
        pltpu.make_async_copy(
            potential.at[pl.ds(sub * 64, 64)], grid_out.at[sub], local_sem.at[1]
        ),
    ]
    for keep in keeps:
        keep.start()
    own_windows = frame.at[pl.ds(0, (SPREAD * SUBS - 1) * TILES)]
    wait_all(recv_sem.at[6], own_windows)
    wait_all(recv_sem.at[5], grid_out.at[pl.ds(0, SUBS - 1)])
    wait_all(send_sem.at[0], got)
    wait_all(send_sem.at[1], told)
    wait_all(send_sem.at[2], outer.at[pl.ds(0, 192)])
    wait_all(send_sem.at[3], back.at[pl.ds(0, count - 1)])
    wait_all(send_sem.at[4], back.at[pl.ds(0, count - 1)])
    wait_all(send_sem.at[5], grid_out.at[pl.ds(0, SUBS - 1)])
    wait_all(send_sem.at[6], own_windows)
    for keep in keeps:
        keep.wait()


def finish_kernel(corner_ref, frame_ref, grid_ref, box_out, grid_out, box, grid, into, out):
    me = lax.axis_index("slab") * SUBS + lax.axis_index("sub")
    offset = corner_ref[0, me] % Z_DEV
    half = BOX * TILES // 2
    moves = [(frame_ref.at[pl.ds(offset * TILES + k * half, half)], box.at[pl.ds(k * half, half)]) for k in range(2)]
    moves.append((grid_ref, grid))
    ends = [box_out.at[pl.ds(0, half)], box_out.at[pl.ds(half, half)], grid_out]
    reads = [pltpu.make_async_copy(a, b, into.at[k]) for k, (a, b) in enumerate(moves)]
    writes = [pltpu.make_async_copy(moves[k][1], ends[k], out.at[k]) for k in range(3)]
    for read in reads:
        read.start()
    for read, write in zip(reads, writes):
        read.wait()
        write.start()
    for write in writes:
        write.wait()


def body(orbitals, occupations, patch_sign, corners, core_span, outer_density):
    count = lax.axis_size("slab") * SUBS
    tables = [jnp.asarray(t) for t in (*cas_table(NX), *cas_table(count))]
    smem = pl.BlockSpec(memory_space=pltpu.SMEM)
    hbm = pl.BlockSpec(memory_space=pl.ANY)
    cores = (REACH * SUBS * 8, 128)
    planes = (SPREAD * SUBS * TILES, 128)
    grid_shape = jax.ShapeDtypeStruct((Z_DEV, NX // SUBS, NY), f32)
    frame, potential = pl.pallas_call(
        whole_kernel,
        out_shape=[
            jax.ShapeDtypeStruct(planes, f32),
            grid_shape,
        ],
        in_specs=[smem] * 4 + [hbm] * 6,
        out_specs=[hbm] * 2,
        scratch_shapes=[
            pltpu.VMEM((BOX * TILES, 128), f32),
            pltpu.VMEM((384, 128), f32),
            pltpu.VMEM(cores, f32),
            pltpu.VMEM((8, 128), jnp.int32),
            pltpu.VMEM(cores, f32),
            pltpu.VMEM((REACH, 128), jnp.int32),
            pltpu.SMEM((REACH, 128), jnp.int32),
            pltpu.VMEM((NX, NY), f32),
            pltpu.VMEM((2, 2 * NX, 128), f32),
            pltpu.VMEM((2, NX + BOX, 128), f32),
            pltpu.VMEM((count, 128), f32),
            pltpu.VMEM((count, 128), f32),
            pltpu.VMEM((count, 128), f32),
            pltpu.VMEM((count, 128), f32),
            pltpu.VMEM((NX, NY), f32),
            pltpu.VMEM((SUBS * BOX, 128), f32),
            pltpu.VMEM(planes, f32),
            pltpu.SemaphoreType.DMA((7,)),
            pltpu.SemaphoreType.DMA((11,)),
            pltpu.SemaphoreType.DMA((9,)),
            pltpu.SemaphoreType.REGULAR,
            pltpu.VMEM((ORB, BOX * BOX * BOX), bf16),
            pltpu.VMEM((NX, NY), bf16),
            pltpu.VMEM((NX, NY), bf16),
            pltpu.VMEM((count, count), bf16),
            pltpu.VMEM((count, count), bf16),
        ],
        compiler_params=pltpu.CompilerParams(collective_id=0, has_side_effects=True),
        name="whole",
    )(core_span, corners.T, occupations, patch_sign.reshape(1, 1), orbitals[0], outer_density, *tables)
    box_potential, potential = pl.pallas_call(
        finish_kernel,
        out_shape=[jax.ShapeDtypeStruct((BOX * TILES, 128), f32), grid_shape],
        in_specs=[smem, hbm, hbm],
        out_specs=[hbm, hbm],
        scratch_shapes=[
            pltpu.VMEM((BOX * TILES, 128), f32),
            pltpu.VMEM(grid_shape.shape, f32),
            pltpu.SemaphoreType.DMA((3,)),
            pltpu.SemaphoreType.DMA((3,)),
        ],
        name="finish",
    )(corners.T, frame, potential)
    return box_potential.reshape(1, BOX * BOX * BOX), potential


def solution(mesh):
    placed = (
        P(("slab", "sub"), None, None),
        P(("slab", "sub"), None),
        P(("slab", "sub")),
        P(),
        P(("slab", "sub"), None),
        P("slab", "sub", None),
    )
    return jax.shard_map(
        body,
        mesh=mesh,
        in_specs=placed,
        out_specs=(P(("slab", "sub"), None), P("slab", "sub", None)),
        check_vma=False,
    )
```
